256 devices in a mesh: rep: 8 (over z_lo, y), shard: 32 (over z_hi, x, core).
Axes of the slice: x: 4, y: 4, z: 8 (z_hi: 4, z_lo: 2; z = z_hi * 2 + z_lo), core: 2. Of those that a mesh axis runs over, the one named last changes fastest.
Arguments:
- activations: bfloat16 [262144, 2048], P(('rep', 'shard')), may hold values from -24 to 24
- cotangents: bfloat16 [262144, 1024], P(('rep', 'shard')), may hold values from -1024 to 1024
- inner_params: float32 [8, 2048, 1024], P('rep', 'shard'), may hold values from -6 to 6
- inner_moment: float32 [8, 2048, 1024], P('rep', 'shard'), may hold values from 0.25 to 4
- outer_params: float32 [2048, 1024], P('shard'), may hold values from -6 to 6
- momentum: float32 [2048, 1024], P('shard'), may hold values from -3 to 3
Outputs:
- new_params: float32 [2048, 1024], P('shard')
- new_momentum: float32 [2048, 1024], P('shard')
- compute_copy: bfloat16 [2048, 1024], replicated
The draws below stay inside these ranges and needn't reach their ends.
All inputs are finite; a program needn't handle non-finite values.
Results may differ from the reference program's by a relative error of at most 0.007.
Values may be sent and summed in bfloat16 or wider, within the bound.
A program may use at most 64 MiB of HBM per device.

```python
import math
import jax
import jax.numpy as jnp
from jax import lax

D = 2048
KV = 1024
TOK_DEV = 1024
REPS = 8
GROUP_TOK = 32768
TOKENS = 262144
N_SHARD = 32


def with_spikes(drawn, own_key, source, target, blocks, factor):
    def block_of(axis_at):
        return (jnp.arange(drawn.shape[axis_at]) // (drawn.shape[axis_at] // blocks)).reshape((-1,) + (1,) * (drawn.ndim - 1 - axis_at))

    first = jax.random.permutation(own_key, blocks)[block_of(target)]
    other_side = (block_of(target) + blocks // 2) % blocks
    return jnp.where((block_of(source) == first) | (block_of(source) == other_side), factor * drawn, drawn)


def shard_levels(stream_key, extent, pieces, least, top_value):
    gain, own = 1.0, jax.random.fold_in(stream_key, 6)
    for position, blocks in pieces:
        heights = jnp.exp(jax.random.uniform(jax.random.fold_in(own, position), (blocks,), jnp.float32, least / len(pieces), top_value / len(pieces)))
        gain = gain * jnp.repeat(heights, extent[position] // blocks).reshape([-1 if axis == position else 1 for axis in range(len(extent))])
    return gain


def bell_draw(stream_key, dims, width, bound, cuts=(), held_as=jnp.bfloat16):
    result = jax.random.normal(stream_key, dims, jnp.float32) * width
    if len(cuts) > 0:
        result = shard_levels(stream_key, dims, cuts, -0.22, 0.18) * result
    return jnp.clip(result, min=-bound, max=bound).astype(held_as)


def noise_with(own_key, dims, spread, reach, pieces, heavy, held_as=jnp.bfloat16):
    array = spread * jax.random.normal(own_key, dims, jnp.float32)
    if pieces:
        array = array * shard_levels(own_key, dims, pieces, -0.22, 0.18)
    return jnp.clip(with_spikes(array, jax.random.fold_in(own_key, 3), *heavy), -reach, reach).astype(held_as)


def setup_inputs(seed: int = 0) -> dict:
    seeds = jax.random.split(jax.random.key(seed), 7)
    activations = noise_with(seeds[0], (TOKENS, D), 1.0, 24.0, ((0, 256),), (0, 1, 256, 6.0))
    cotangents = bell_draw(seeds[1], (TOKENS, KV), (GROUP_TOK ** 0.5), 1024.0, ((0, 256),))
    inner_params = bell_draw(seeds[2], (REPS, D, KV), 1.0, 6.0, ((0, 8), (1, 32)), jnp.float32)
    inner_moment = jnp.clip(jnp.exp(math.log(4.0) - 2.7725887 * jax.random.uniform(seeds[3], (REPS, D, KV), jnp.float32) ** shard_levels(seeds[3], (REPS, D, KV), ((0, 8), (1, 32)), -0.2, 0.2)), 0.25, 4.0)
    outer_params = bell_draw(seeds[4], (D, KV), 1.0, 6.0, ((0, 32),), jnp.float32)
    momentum = bell_draw(seeds[5], (D, KV), 0.5, 3.0, ((0, 32),), jnp.float32)
    return dict(activations=activations, cotangents=cotangents, inner_params=inner_params, inner_moment=inner_moment, outer_params=outer_params, momentum=momentum)


outer_rate = 0.7
inertia = 0.9
inner_rate = 0.3
epsilon = 1e-08

def reference(activations, cotangents, inner_params, inner_moment, outer_params, momentum):
    group_tok = TOK_DEV * N_SHARD
    delta_total = jnp.zeros(outer_params.shape, jnp.float32)
    for replica in range(REPS):
        rows_act = activations[replica * group_tok:(replica + 1) * group_tok]
        rows_cot = cotangents[replica * group_tok:(replica + 1) * group_tok]
        summed = lax.dot_general(rows_act, rows_cot, (((0,), (0,)), ((), ())), preferred_element_type=jnp.float32)
        mean_grad = summed / group_tok
        replica_params = inner_params[replica] - inner_rate * mean_grad / (jnp.sqrt(inner_moment[replica]) + epsilon)
        delta_total = delta_total + (outer_params - replica_params)
    pseudo_grad = delta_total / REPS
    new_momentum = inertia * momentum + pseudo_grad
    new_params = outer_params - outer_rate * (pseudo_grad + inertia * new_momentum)
    return (new_params, new_momentum, new_params.astype(jnp.bfloat16))
```

```python
import functools

import jax
import jax.numpy as jnp
from jax import lax
from jax.experimental import pallas as pl
from jax.experimental.pallas import tpu as pltpu
from jax.sharding import Mesh
from jax.sharding import PartitionSpec as P

MESH = pl.DeviceIdType.MESH
AXES = ("zl", "y", "zh", "x", "c")
SIZE = {"zl": 2, "y": 4, "zh": 4, "x": 4, "c": 2}
REP = ("zl", "y")
SHARD = ("zh", "x", "c")
BF16, F32 = jnp.bfloat16, jnp.float32

outer_rate = 0.7
inertia = 0.9
inner_rate = 0.3
epsilon = 1e-08

NQ = 2
SEMS = 96


def kernel(
    act, cot, inner, moment, outer, mom, new_p, new_m, cc,
    a_buf, b_buf, grad, core_in, two_in, direct_in, fwd_in, weight, y_own, y_in, z_own, z_in,
    base, base_in, base_sum, base_y, nm, load_sem, ss, rs,
):
    zl, y, zh, x, c = (lax.axis_index(a) for a in AXES)
    at = {"zl": zl, "y": y, "zh": zh, "x": x, "c": c}

    def shift(axis, d):
        return {axis: lax.rem(at[axis] + d, SIZE[axis])}

    z = zh * 2 + zl

    def z_shift(d):
        there = lax.rem(z + d, 8)
        return {"zh": there // 2, "zl": lax.rem(there, 2)}

    core = {"c": 1 - c}
    pair = {"zl": 1 - zl}

    loads = [pltpu.make_async_copy(cot, b_buf, load_sem.at[16])]
    steps = (2, 1, 3, 0)
    for j, step in enumerate(steps):
        there = lax.rem(x + step, 4)
        for h in range(4):
            columns = pl.ds(pl.multiple_of(h * 512 + there * 128, 128), 128)
            loads.append(
                pltpu.make_async_copy(
                    act.at[:, columns], a_buf.at[j, :, pl.ds(h * 128, 128)], load_sem.at[j * 4 + h]
                )
            )
    for load in loads:
        load.start()

    barrier = pltpu.get_barrier_semaphore()
    peers = [core] + [shift("x", d) for d in (1, 2, 3)] + [shift("y", d) for d in (1, 2, 3)]
    peers += [z_shift(d) for d in range(1, 8)]
    for peer in peers:
        pl.semaphore_signal(barrier, inc=1, device_id=peer, device_id_type=MESH)

    factor = (inner_rate / (8 * 32768)) / (jnp.sqrt(moment[0]) + epsilon)
    for q in range(NQ):
        weight[q, zh] = factor[q * 32 : q * 32 + 32].astype(BF16)
    for t in range(4):
        for s in range(2):
            cols = slice(t * 256 + s * 128, t * 256 + s * 128 + 128)
            base[s, t] = outer[:, cols] - inner[0, :, cols]

    pl.semaphore_wait(barrier, len(peers))

    count = [0]
    sent = []

    def send(src, dst, peer):
        i = count[0]
        count[0] += 1
        copy = pltpu.make_async_remote_copy(
            src, dst, ss.at[i], rs.at[i], device_id=peer, device_id_type=MESH
        )
        copy.start()
        sent.append(copy)
        return copy

    w_copies = [send(weight.at[:, zh], weight.at[:, zh], shift("zh", d)) for d in (1, 2, 3)]
    base_copy = send(base.at[1 - zl], base_in, pair)

    core_copies = []
    loads[0].wait()

    def product(j):
        for load in loads[1 + 4 * j : 5 + 4 * j]:
            load.wait()
        for n in range(2):
            cols = slice(n * 512, n * 512 + 512)
            value = lax.dot_general(
                a_buf[j], b_buf[:, cols], (((0,), (0,)), ((), ())), preferred_element_type=F32
            ).astype(BF16)
            for h in range(4):
                for k in range(2):
                    for q in range(NQ):
                        row = h * 128 + k * 64 + q * 32
                        grad[j, k, q, h, :, cols] = value[row : row + 32]
        core_copies.append(send(grad.at[j, 1 - c], core_in.at[j], core))

    def chip_sum(j):
        core_copies[j].wait_recv()
        for q in range(NQ):
            for h in range(4):
                grad[j, c, q, h] = grad[j, c, q, h] + core_in[j, q, h]

    lo, hi = pl.ds(0, 2), pl.ds(2, 2)
    right, left = shift("x", 1), shift("x", 3)
    two, direct, fwd = {}, {}, {}

    def send_two(q):
        two[q] = (
            send(grad.at[0, c, q, lo], two_in.at[q, 0], left),
            send(grad.at[0, c, q, hi], two_in.at[q, 1], right),
        )

    def send_right(q):
        direct[q, 0] = send(grad.at[1, c, q, lo], direct_in.at[q, 0], right)

    def send_left(q):
        direct[q, 1] = send(grad.at[2, c, q, hi], direct_in.at[q, 1], left)

    def forward(q):
        two[q][1].wait_recv()
        for h in range(2):
            grad[1, c, q, 2 + h] = grad[1, c, q, 2 + h] + two_in[q, 1, h]
        right_copy = send(grad.at[1, c, q, hi], fwd_in.at[q, 1], right)
        two[q][0].wait_recv()
        for h in range(2):
            grad[2, c, q, h] = grad[2, c, q, h] + two_in[q, 0, h]
        fwd[q] = (send(grad.at[2, c, q, lo], fwd_in.at[q, 0], left), right_copy)

    y_copies = {}

    def finish_x(q):
        for copy in (direct[q, 0], direct[q, 1], *fwd[q]):
            copy.wait_recv()
        for h in range(4):
            half, place = h // 2, h % 2
            total = grad[3, c, q, h].astype(F32) + direct_in[q, half, place].astype(F32)
            total = total + fwd_in[q, half, place].astype(F32)
            total = (total * weight[q, h].astype(F32)).astype(BF16)
            for t in range(4):
                y_own[q, t, h] = total[:, t * 256 : t * 256 + 256]
        y_copies[q] = [
            send(y_own.at[q, lax.rem(y + d, 4)], y_in.at[q, d - 1], shift("y", d)) for d in (1, 3, 2)
        ]

    z_copies = {}

    def finish_y(q):
        for copy in y_copies[q]:
            copy.wait_recv()
        for h in range(4):
            total = y_own[q, y, h].astype(F32) + y_in[q, 0, h].astype(F32)
            total = total + y_in[q, 1, h].astype(F32) + y_in[q, 2, h].astype(F32)
            for s in range(2):
                z_own[q, h * 2 + s] = total[:, s * 128 : s * 128 + 128].astype(BF16)
        z_copies[q] = [
            send(z_own.at[q, lax.rem(z + d, 8)], z_in.at[q, d - 1], z_shift(d))
            for d in (4, 3, 5, 2, 6, 1, 7)
        ]

    product(0)
    product(1)
    chip_sum(0)
    two_sent = send_two(0)
    product(2)
    chip_sum(1)
    send_right(0)
    product(3)
    chip_sum(2)
    send_left(0)
    base_copy.wait_recv()
    for t in range(4):
        base_sum[t] = base[zl, t] + base_in[t]
    base_copies = [
        send(base_sum.at[lax.rem(y + d, 4)], base_y.at[d - 1], shift("y", d)) for d in (1, 2, 3)
    ]
    chip_sum(3)
    forward(0)
    send_two(1)
    send_right(1)
    send_left(1)
    for copy in w_copies:
        copy.wait_recv()
    finish_x(0)
    for copy in base_copies:
        copy.wait_recv()
    pseudo_base = base_sum[y] + base_y[0] + base_y[1] + base_y[2]
    forward(1)
    finish_y(0)
    finish_x(1)
    finish_y(1)

    cut = pl.ds(pl.multiple_of(y * 256 + zl * 128, 128), 128)
    y_cut = pl.ds(pl.multiple_of(y * 256, 128), 256)
    for q in range(NQ):
        for copy in z_copies[q]:
            copy.wait_recv()
        rows = pl.ds(q * 32, 32)
        total = z_own[q, z].astype(F32)
        for d in range(7):
            total = total + z_in[q, d].astype(F32)
        pseudo = pseudo_base[q * 32 : q * 32 + 32] / 8 + total
        fresh_m = inertia * mom[rows, cut] + pseudo
        fresh_p = outer[rows, cut] - outer_rate * (pseudo + inertia * fresh_m)
        cc[zh, x, c, rows, cut] = fresh_p.astype(BF16)
        nm[rows, cut] = fresh_m.astype(BF16)

    own = cc.at[zh, x, c, :, cut]
    far = [send(own, own, z_shift(d)) for d in (4, 3, 5, 2, 6, 1, 7)]
    nm_pair = send(nm.at[:, cut], nm.at[:, cut], pair)
    for copy in far:
        copy.wait_recv()
    rows0, rows1 = pl.ds(0, 32), pl.ds(32, 32)
    part0 = cc.at[:, x, c, rows0, y_cut]
    part1 = cc.at[:, x, c, rows1, y_cut]
    mid0 = [send(part0, part0, shift("y", d)) for d in (1, 3, 2)]
    mid1 = [send(part1, part1, shift("x", d)) for d in (1, 3, 2)]
    nm_pair.wait_recv()
    nm_y = [send(nm.at[:, y_cut], nm.at[:, y_cut], shift("y", d)) for d in (1, 3, 2)]

    up, down = shift("y", 1), shift("y", 3)
    last = []

    def core_send(part):
        last.append(send(part, part, core))

    def x_part(place, rows):
        return cc.at[:, place, c, rows]

    def y_part(place, rows):
        return cc.at[:, :, c, rows, pl.ds(pl.multiple_of(place * 256, 128), 256)]

    for copy in mid0:
        copy.wait_recv()
    mine0 = x_part(x, rows0)
    ring0 = [send(mine0, mine0, right), send(mine0, mine0, left)]
    for copy in mid1:
        copy.wait_recv()
    mine1 = y_part(y, rows1)
    ring1 = [send(mine1, mine1, up), send(mine1, mine1, down)]
    core_send(mine0)
    core_send(mine1)
    x_left, x_right = lax.rem(x + 3, 4), lax.rem(x + 1, 4)
    y_down, y_up = lax.rem(y + 3, 4), lax.rem(y + 1, 4)
    ring0[0].wait_recv()
    piece = x_part(x_left, pl.ds(0, 16))
    tail = [send(piece, piece, right)]
    ring0[1].wait_recv()
    piece = x_part(x_right, pl.ds(16, 16))
    tail.append(send(piece, piece, left))
    ring1[0].wait_recv()
    piece = y_part(y_down, pl.ds(32, 16))
    tail.append(send(piece, piece, up))
    ring1[1].wait_recv()
    piece = y_part(y_up, pl.ds(48, 16))
    tail.append(send(piece, piece, down))
    core_send(x_part(x_left, rows0))
    core_send(x_part(x_right, rows0))
    core_send(y_part(y_down, rows1))
    core_send(y_part(y_up, rows1))
    for copy in nm_y:
        copy.wait_recv()
    new_m[...] = nm[...].astype(F32)
    x_far, y_far = lax.rem(x + 2, 4), lax.rem(y + 2, 4)
    tail[0].wait_recv()
    core_send(x_part(x_far, pl.ds(0, 16)))
    tail[1].wait_recv()
    core_send(x_part(x_far, pl.ds(16, 16)))
    tail[2].wait_recv()
    core_send(y_part(y_far, pl.ds(32, 16)))
    tail[3].wait_recv()
    core_send(y_part(y_far, pl.ds(48, 16)))
    new_p[...] = cc[zh, x, c].astype(F32)
    for copy in last:
        copy.wait_recv()
    for copy in sent:
        copy.wait_send()


def per_device(activations, cotangents, inner_params, inner_moment, outer_params, momentum):
    vmem = pl.BlockSpec(memory_space=pltpu.VMEM)
    hbm = pl.BlockSpec(memory_space=pl.ANY)
    new_p, new_m, cc = pl.pallas_call(
        kernel,
        out_shape=(
            jax.ShapeDtypeStruct((64, 1024), F32),
            jax.ShapeDtypeStruct((64, 1024), F32),
            jax.ShapeDtypeStruct((4, 4, 2, 64, 1024), BF16),
        ),
        in_specs=[hbm, hbm, vmem, vmem, vmem, vmem],
        out_specs=(vmem, vmem, vmem),
        scratch_shapes=[
            pltpu.VMEM((4, 1024, 512), BF16),
            pltpu.VMEM((1024, 1024), BF16),
            pltpu.VMEM((4, 2, NQ, 4, 32, 1024), BF16),
            pltpu.VMEM((4, NQ, 4, 32, 1024), BF16),
            pltpu.VMEM((NQ, 2, 2, 32, 1024), BF16),
            pltpu.VMEM((NQ, 2, 2, 32, 1024), BF16),
            pltpu.VMEM((NQ, 2, 2, 32, 1024), BF16),
            pltpu.VMEM((NQ, 4, 32, 1024), BF16),
            pltpu.VMEM((NQ, 4, 4, 32, 256), BF16),
            pltpu.VMEM((NQ, 3, 4, 32, 256), BF16),
            pltpu.VMEM((NQ, 8, 32, 128), BF16),
            pltpu.VMEM((NQ, 7, 32, 128), BF16),
            pltpu.VMEM((2, 4, 64, 128), F32),
            pltpu.VMEM((4, 64, 128), F32),
            pltpu.VMEM((4, 64, 128), F32),
            pltpu.VMEM((3, 64, 128), F32),
            pltpu.VMEM((64, 1024), BF16),
            pltpu.SemaphoreType.DMA((17,)),
            pltpu.SemaphoreType.DMA((SEMS,)),
            pltpu.SemaphoreType.DMA((SEMS,)),
        ],
        compiler_params=pltpu.CompilerParams(
            collective_id=0, has_side_effects=True, vmem_limit_bytes=56 * 2**20
        ),
    )(activations, cotangents, inner_params, inner_moment, outer_params, momentum)
    return new_p, new_m, cc.reshape(2048, 1024)


def solution(mesh):
    split = Mesh(mesh.devices.reshape(*(SIZE[a] for a in AXES)), AXES)
    return jax.shard_map(
        per_device,
        mesh=split,
        in_specs=(
            P(AXES, None),
            P(AXES, None),
            P(REP, SHARD, None),
            P(REP, SHARD, None),
            P(SHARD, None),
            P(SHARD, None),
        ),
        out_specs=(P(SHARD, None), P(SHARD, None), P()),
        check_vma=False,
    )
```

```python
import functools

import jax
import jax.numpy as jnp
from jax import lax
from jax.experimental import pallas as pl
from jax.experimental.pallas import tpu as pltpu
from jax.sharding import Mesh
from jax.sharding import PartitionSpec as P

MESH = pl.DeviceIdType.MESH
AXES = ("zl", "y", "zh", "x", "c")
SIZE = {"zl": 2, "y": 4, "zh": 4, "x": 4, "c": 2}
REP = ("zl", "y")
SHARD = ("zh", "x", "c")
BF16, F32 = jnp.bfloat16, jnp.float32

outer_rate = 0.7
inertia = 0.9
inner_rate = 0.3
epsilon = 1e-08

NQ = 4
COLS = 1024 // NQ
SEMS = 200
STEPS = (2, 1, 3, 0)
FAR = (4, 3, 5, 2, 6, 1, 7)


def kernel(
    act, cot, inner_h, moment_h, outer_h, mom_h, nm, cc,
    a_buf, b_buf, grad, core_in, two_in, direct_in, fwd_in, weight, y_own, y_in, z_own, z_in,
    inner, moment, outer, mom, base, base_in, base_sum, base_y, load_sem, ss, rs,
):
    zl, y, zh, x, c = (lax.axis_index(a) for a in AXES)
    at = {"zl": zl, "y": y, "zh": zh, "x": x, "c": c}

    def shift(axis, d):
        return {axis: lax.rem(at[axis] + d, SIZE[axis])}

    z = zh * 2 + zl

    def z_shift(d):
        there = lax.rem(z + d, 8)
        return {"zh": there // 2, "zl": lax.rem(there, 2)}

    core = {"c": 1 - c}
    pair = {"zl": 1 - zl}
    right, left = shift("x", 1), shift("x", 3)

    barrier = pltpu.get_barrier_semaphore()
    peers = [core] + [shift("x", d) for d in (1, 2, 3)] + [shift("y", d) for d in (1, 2, 3)]
    peers += [z_shift(d) for d in range(1, 8)]
    for peer in peers:
        pl.semaphore_signal(barrier, inc=1, device_id=peer, device_id_type=MESH)

    loads = []

    def load(src, dst):
        copy = pltpu.make_async_copy(src, dst, load_sem.at[len(loads)])
        copy.start()
        loads.append(copy)

    a_loads, b_loads = {}, {}

    def load_a(j):
        there = lax.rem(x + STEPS[j], 4)
        for h in range(4):
            columns = pl.ds(pl.multiple_of(h * 512 + there * 128, 128), 128)
            load(act.at[:, columns], a_buf.at[j, :, pl.ds(h * 128, 128)])
        a_loads[j] = loads[-4:]

    def load_b(p):
        load(cot.at[:, pl.ds(p * 512, 512)], b_buf.at[p])
        b_loads[p] = loads[-1:]

    load_a(0)
    load_b(0)
    load_a(1)
    load_a(2)
    load(moment_h, moment)
    moment_load = loads[-1]
    load(inner_h, inner)
    load(outer_h, outer)
    base_loads = loads[-2:]
    load_a(3)
    load_b(1)
    load(mom_h, mom)
    mom_load = loads[-1]

    count = [0]
    sent = []

    def send(src, dst, peer):
        i = count[0]
        count[0] += 1
        copy = pltpu.make_async_remote_copy(
            src, dst, ss.at[i], rs.at[i], device_id=peer, device_id_type=MESH
        )
        copy.start()
        sent.append(copy)
        return copy

    def arrive(copies):
        for copy in copies:
            copy.wait_recv()

    core_copies = {}

    def product(j, p):
        for copy in a_loads.pop(j, []) + b_loads.pop(p, []):
            copy.wait()
        value = lax.dot_general(
            a_buf[j], b_buf[p], (((0,), (0,)), ((), ())), preferred_element_type=F32
        ).astype(BF16)
        for q in range(2):
            for h in range(4):
                for k in range(2):
                    row = h * 128 + k * 64
                    part = value[row : row + 64, q * COLS : q * COLS + COLS]
                    grad[j, k, 2 * p + q, h] = part

    def core_share(j, p):
        for q in (2 * p, 2 * p + 1):
            core_copies[j, q] = send(grad.at[j, 1 - c, q], core_in.at[j, q], core)

    def chip_sum(j, q):
        core_copies[j, q].wait_recv()
        for h in range(4):
            grad[j, c, q, h] = grad[j, c, q, h] + core_in[j, q, h]

    lo, hi = pl.ds(0, 2), pl.ds(2, 2)
    two, direct, fwd, y_copies, z_copies = {}, {}, {}, {}, {}
    far, mid0, mid1, last0, last1 = {}, {}, {}, {}, {}

    def send_two(q):
        two[q] = (
            send(grad.at[0, c, q, lo], two_in.at[q, 0], left),
            send(grad.at[0, c, q, hi], two_in.at[q, 1], right),
        )

    def send_right(q):
        direct[q, 0] = send(grad.at[1, c, q, lo], direct_in.at[q, 0], right)

    def send_left(q):
        direct[q, 1] = send(grad.at[2, c, q, hi], direct_in.at[q, 1], left)

    def forward(q):
        two[q][1].wait_recv()
        for h in range(2):
            grad[1, c, q, 2 + h] = grad[1, c, q, 2 + h] + two_in[q, 1, h]
        right_copy = send(grad.at[1, c, q, hi], fwd_in.at[q, 1], right)
        two[q][0].wait_recv()
        for h in range(2):
            grad[2, c, q, h] = grad[2, c, q, h] + two_in[q, 0, h]
        fwd[q] = (send(grad.at[2, c, q, lo], fwd_in.at[q, 0], left), right_copy)

    def finish_x(q):
        arrive(w_copies[q])
        arrive((direct[q, 0], direct[q, 1], *fwd[q]))
        for h in range(4):
            half, place = h // 2, h % 2
            total = grad[3, c, q, h].astype(F32) + direct_in[q, half, place].astype(F32)
            total = total + fwd_in[q, half, place].astype(F32)
            total = (total * weight[q, h].astype(F32)).astype(BF16)
            for t in range(4):
                y_own[q, t, h] = total[t * 16 : t * 16 + 16]
        y_copies[q] = [
            send(y_own.at[q, lax.rem(y + d, 4)], y_in.at[q, d - 1], shift("y", d)) for d in (2, 1, 3)
        ]

    def finish_y(q):
        arrive(y_copies[q])
        for h in range(4):
            total = y_own[q, y, h].astype(F32) + y_in[q, 0, h].astype(F32)
            total = total + y_in[q, 1, h].astype(F32) + y_in[q, 2, h].astype(F32)
            for s in range(2):
                z_own[q, h * 2 + s] = total[:, s * 128 : s * 128 + 128].astype(BF16)
        z_copies[q] = [
            send(z_own.at[q, lax.rem(z + d, 8)], z_in.at[q, d - 1], z_shift(d)) for d in FAR
        ]

    rows = pl.ds(pl.multiple_of(y * 16, 16), 16)

    def finish_z(q):
        arrive(z_copies[q])
        cut = pl.ds(pl.multiple_of(q * COLS + zl * 128, 128), 128)
        total = z_own[q, z].astype(F32)
        for d in range(7):
            total = total + z_in[q, d].astype(F32)
        pseudo = base_y[3, :, q * 128 : q * 128 + 128] / 8 + total
        fresh_m = inertia * mom[rows, cut] + pseudo
        fresh_p = outer[rows, cut] - outer_rate * (pseudo + inertia * fresh_m)
        cc[zh, x, c, rows, cut] = fresh_p.astype(BF16)
        nm[y, zl, :, q * 128 : q * 128 + 128] = fresh_m.astype(BF16)
        own = cc.at[zh, x, c, rows, cut]
        far[q] = [send(own, own, z_shift(d)) for d in FAR]

    def columns_of(q):
        return pl.ds(q * COLS, COLS)

    def gather_mid(q):
        arrive(far[q])
        part0 = cc.at[lo, x, c, rows, columns_of(q)]
        part1 = cc.at[hi, x, c, rows, columns_of(q)]
        mid0[q] = [send(part0, part0, shift("y", d)) for d in (2, 1, 3)]
        mid1[q] = [send(part1, part1, shift("x", d)) for d in (2, 1, 3)]

    def x_part(q, d):
        return cc.at[lo, lax.rem(x + d, 4), c, :, columns_of(q)]

    def y_part(q, d):
        place = pl.ds(pl.multiple_of(lax.rem(y + d, 4) * 16, 16), 16)
        return cc.at[hi, :, c, place, columns_of(q)]

    shared = []

    def core_send(part):
        shared.append(send(part, part, core))

    def gather_last(q):
        arrive(mid0[q])
        part0 = x_part(q, 0)
        last0[q] = [(d, send(part0, part0, shift("x", d))) for d in (2, 1, 3)]
        arrive(mid1[q])
        part1 = y_part(q, 0)
        last1[q] = [(d, send(part1, part1, shift("y", d))) for d in (2, 1, 3)]
        if q == NQ - 1:
            core_send(part0)
            core_send(part1)

    def gather_core(q):
        if q < NQ - 1:
            arrive([copy for _, copy in last0[q] + last1[q]])
            core_send(cc.at[:, :, c, :, columns_of(q)])
            return
        for i in (1, 2, 0):
            d, copy = last0[q][i]
            copy.wait_recv()
            core_send(x_part(q, 4 - d))
            d, copy = last1[q][i]
            copy.wait_recv()
            core_send(y_part(q, 4 - d))

    def make(*pairs):
        for j, p in pairs:
            product(j, p)
            core_share(j, p)

    product(0, 0)
    pl.semaphore_wait(barrier, len(peers))
    core_share(0, 0)
    make((1, 0))
    chip_sum(0, 0)
    send_two(0)
    chip_sum(0, 1)
    send_two(1)
    make((2, 0))
    chip_sum(1, 0)
    send_right(0)
    moment_load.wait()
    factor = (inner_rate / (8 * 32768)) / (jnp.sqrt(moment[0]) + epsilon)
    w_copies = {}

    def share_weight(q):
        part = weight.at[q, zh]
        w_copies[q] = [send(part, part, shift("zh", d)) for d in (2, 1, 3)]

    for q in range(NQ):
        weight[q, zh] = factor[:, q * COLS : q * COLS + COLS].astype(BF16)
    share_weight(0)
    for copy in base_loads:
        copy.wait()
    for t in range(4):
        for s in range(2):
            for q in range(NQ):
                cols = slice(q * COLS + s * 128, q * COLS + s * 128 + 128)
                part = slice(t * 16, t * 16 + 16)
                base[s, t, :, q * 128 : q * 128 + 128] = outer[part, cols] - inner[0, part, cols]
    base_copy = send(base.at[1 - zl], base_in, pair)
    for q in range(1, NQ):
        share_weight(q)
    chip_sum(2, 0)
    send_left(0)
    make((3, 0), (0, 1))
    for j in (1, 2, 3):
        chip_sum(j, 1)
    chip_sum(3, 0)
    forward(0)
    chip_sum(0, 2)
    send_two(2)
    send_right(1)
    send_left(1)
    make((1, 1))
    forward(1)
    chip_sum(0, 3)
    send_two(3)
    make((2, 1))
    chip_sum(1, 2)
    send_right(2)
    make((3, 1))
    chip_sum(2, 2)
    send_left(2)
    for j, q in ((3, 2), (1, 3), (2, 3), (3, 3)):
        chip_sum(j, q)
    mom_load.wait()

    held = {}

    def base_pair():
        base_copy.wait_recv()
        for t in range(4):
            base_sum[t] = base[zl, t] + base_in[t]
        held["base"] = [
            send(base_sum.at[lax.rem(y + d, 4)], base_y.at[d - 1], shift("y", d)) for d in (2, 1, 3)
        ]

    def base_total():
        arrive(held["base"])
        base_y[3] = base_sum[y] + base_y[0] + base_y[1] + base_y[2]

    def fwd_and_next(q):
        forward(q)
        if q == 2:
            send_right(3)
            send_left(3)

    def nm_pair():
        part = nm.at[y, zl]
        held["nm"] = send(part, part, pair)

    def nm_y():
        held["nm"].wait_recv()
        part = nm.at[y]
        held["nm_y"] = [send(part, part, shift("y", d)) for d in (2, 1, 3)]

    done = (7.6, 11.8, 16.0, 19.0)
    events = [(9.0, fwd_and_next, (2,)), (13.2, fwd_and_next, (3,))]
    events += [(11.3, base_pair, ()), (15.5, base_total, ())]
    stages = (finish_x, finish_y, finish_z, gather_mid, gather_last, gather_core)
    for q in range(NQ):
        waits = (0, 3.5, 8, 12.5, 16, 22) if q < NQ - 1 else (0, 3, 6.8, 10.5, 13.5, 18.5)
        events += [(done[q] + wait, stage, (q,)) for wait, stage in zip(waits, stages)]
    events += [(done[-1] + 7.1, nm_pair, ()), (done[-1] + 11.1, nm_y, ())]
    for _, stage, operands in sorted(events, key=lambda event: event[0]):
        stage(*operands)
    arrive(held["nm_y"])
    arrive(shared)
    for copy in sent:
        copy.wait_send()


def write(nm, cc, new_p, new_m, out, buf_p, buf_m, sem):
    zh, x, c = (lax.axis_index(a) for a in SHARD)
    copies = [pltpu.make_async_copy(cc, out, sem.at[0])]
    copies[0].start()
    buf_p[...] = cc[zh, x, c].astype(F32)
    copies.append(pltpu.make_async_copy(buf_p, new_p, sem.at[1]))
    copies[1].start()
    for t in range(4):
        for s in range(2):
            for q in range(NQ):
                cols = slice(q * COLS + s * 128, q * COLS + s * 128 + 128)
                value = nm[t, s, :, q * 128 : q * 128 + 128].astype(F32)
                buf_m[t * 16 : t * 16 + 16, cols] = value
    copies.append(pltpu.make_async_copy(buf_m, new_m, sem.at[2]))
    copies[2].start()
    for copy in copies:
        copy.wait()


def per_device(activations, cotangents, inner_params, inner_moment, outer_params, momentum):
    vmem = pl.BlockSpec(memory_space=pltpu.VMEM)
    hbm = pl.BlockSpec(memory_space=pltpu.HBM)
    whole = (4, 4, 2, 64, 1024)
    nm, cc = pl.pallas_call(
        kernel,
        out_shape=(pltpu.VMEM((4, 2, 16, NQ * 128), BF16), pltpu.VMEM(whole, BF16)),
        in_specs=[hbm] * 6,
        out_specs=(vmem, vmem),
        scratch_shapes=[
            pltpu.VMEM((4, 1024, 512), BF16),
            pltpu.VMEM((2, 1024, 512), BF16),
            pltpu.VMEM((4, 2, NQ, 4, 64, COLS), BF16),
            pltpu.VMEM((4, NQ, 4, 64, COLS), BF16),
            pltpu.VMEM((NQ, 2, 2, 64, COLS), BF16),
            pltpu.VMEM((NQ, 2, 2, 64, COLS), BF16),
            pltpu.VMEM((NQ, 2, 2, 64, COLS), BF16),
            pltpu.VMEM((NQ, 4, 64, COLS), BF16),
            pltpu.VMEM((NQ, 4, 4, 16, COLS), BF16),
            pltpu.VMEM((NQ, 3, 4, 16, COLS), BF16),
            pltpu.VMEM((NQ, 8, 16, 128), BF16),
            pltpu.VMEM((NQ, 7, 16, 128), BF16),
            pltpu.VMEM((1, 64, 1024), F32),
            pltpu.VMEM((1, 64, 1024), F32),
            pltpu.VMEM((64, 1024), F32),
            pltpu.VMEM((64, 1024), F32),
            pltpu.VMEM((2, 4, 16, NQ * 128), F32),
            pltpu.VMEM((4, 16, NQ * 128), F32),
            pltpu.VMEM((4, 16, NQ * 128), F32),
            pltpu.VMEM((4, 16, NQ * 128), F32),
            pltpu.SemaphoreType.DMA((32,)),
            pltpu.SemaphoreType.DMA((SEMS,)),
            pltpu.SemaphoreType.DMA((SEMS,)),
        ],
        compiler_params=pltpu.CompilerParams(
            collective_id=0, has_side_effects=True, vmem_limit_bytes=61100 * 1024
        ),
    )(activations, cotangents, inner_params, inner_moment, outer_params, momentum)
    new_p, new_m, out = pl.pallas_call(
        write,
        out_shape=(
            jax.ShapeDtypeStruct((64, 1024), F32),
            jax.ShapeDtypeStruct((64, 1024), F32),
            jax.ShapeDtypeStruct(whole, BF16),
        ),
        in_specs=[vmem, vmem],
        out_specs=(hbm, hbm, hbm),
        scratch_shapes=[
            pltpu.VMEM((64, 1024), F32),
            pltpu.VMEM((64, 1024), F32),
            pltpu.SemaphoreType.DMA((3,)),
        ],
        compiler_params=pltpu.CompilerParams(vmem_limit_bytes=8 * 2**20),
    )(nm, cc)
    return new_p, new_m, out.reshape(2048, 1024)


def solution(mesh):
    split = Mesh(mesh.devices.reshape(*(SIZE[a] for a in AXES)), AXES)
    return jax.shard_map(
        per_device,
        mesh=split,
        in_specs=(
            P(AXES, None),
            P(AXES, None),
            P(REP, SHARD, None),
            P(REP, SHARD, None),
            P(SHARD, None),
            P(SHARD, None),
        ),
        out_specs=(P(SHARD, None), P(SHARD, None), P()),
        check_vma=False,
    )
```

```python
import functools

import jax
import jax.numpy as jnp
from jax import lax
from jax.experimental import pallas as pl
from jax.experimental.pallas import tpu as pltpu
from jax.sharding import Mesh
from jax.sharding import PartitionSpec as P

MESH = pl.DeviceIdType.MESH
AXES = ("zl", "y", "zh", "x", "c")
SIZE = {"zl": 2, "y": 4, "zh": 4, "x": 4, "c": 2}
REP = ("zl", "y")
SHARD = ("zh", "x", "c")
BF16, F32 = jnp.bfloat16, jnp.float32

outer_rate = 0.7
inertia = 0.9
inner_rate = 0.3
epsilon = 1e-08

NQ = 4
COLS = 1024 // NQ
RING = (0, 2, 3)
FIRST_Z = 1
ORDER = ("X0", "F3", "Y0", "cs", "zf", "X2", "X3", "Y2", "bt", "Z0", "Y3", "zs", "Z2", "M0", "zx", "Z3", "M2", "L0", "Z1", "np", "M3", "L2", "G0", "M1", "ny", "L3", "G2", "L1", "C0", "C2", "C3", "C1")
DIRECT = (1, 3)
SEMS = 200
STEPS = (2, 1, 3, 0)
FAR = (4, 3, 5, 2, 6, 1, 7)


def kernel(
    act, cot, inner_h, moment_h, outer_h, mom_h, nm, cc,
    a_buf, b_buf, grad, core_in, two_in, direct_in, fwd_in, weight, y_own, y_in, z_own, z_in,
    inner, moment, outer, mom, base, base_in, base_sum, base_far, own_factor, zh_two_in, zh_direct_in, zh_fwd_in, zh_sum, zx_in, rep_own, load_sem, ss, rs,
):
    zl, y, zh, x, c = (lax.axis_index(a) for a in AXES)
    at = {"zl": zl, "y": y, "zh": zh, "x": x, "c": c}

    def shift(axis, d):
        return {axis: lax.rem(at[axis] + d, SIZE[axis])}

    z = zh * 2 + zl

    def z_shift(d):
        there = lax.rem(z + d, 8)
        return {"zh": there // 2, "zl": lax.rem(there, 2)}

    core = {"c": 1 - c}
    pair = {"zl": 1 - zl}
    right, left = shift("x", 1), shift("x", 3)

    barrier = pltpu.get_barrier_semaphore()
    peers = [core, right, left] + [shift("y", d) for d in (1, 2, 3)]
    peers += [z_shift(d) for d in (1, 2, 6, 7)]
    for peer in peers:
        pl.semaphore_signal(barrier, inc=1, device_id=peer, device_id_type=MESH)

    loads = []

    def load(src, dst):
        copy = pltpu.make_async_copy(src, dst, load_sem.at[len(loads)])
        copy.start()
        loads.append(copy)

    a_loads, b_loads = {}, {}

    def load_a(j):
        there = lax.rem(x + STEPS[j], 4)
        for h in range(4):
            columns = pl.ds(pl.multiple_of(h * 512 + there * 128, 128), 128)
            load(act.at[:, columns], a_buf.at[j, :, pl.ds(h * 128, 128)])
        a_loads[j] = loads[-4:]

    def load_b(p):
        load(cot.at[:, pl.ds(p * 512, 512)], b_buf.at[p])
        b_loads[p] = loads[-1:]

    load_a(0)
    load_b(0)
    load(moment_h, moment)
    moment_load = loads[-1]
    load_a(1)
    load_a(2)
    load(inner_h, inner)
    load(outer_h, outer)
    base_loads = loads[-2:]
    load_a(3)
    load_b(1)
    load(mom_h, mom)
    mom_load = loads[-1]

    count = [0]
    sent = []

    def send(src, dst, peer):
        i = count[0]
        count[0] += 1
        copy = pltpu.make_async_remote_copy(
            src, dst, ss.at[i], rs.at[i], device_id=peer, device_id_type=MESH
        )
        copy.start()
        sent.append(copy)
        return copy

    def arrive(copies):
        for copy in copies:
            copy.wait_recv()

    core_copies = {}

    def product(j, p):
        for copy in a_loads.pop(j, []) + b_loads.pop(p, []):
            copy.wait()
        value = lax.dot_general(
            a_buf[j], b_buf[p], (((0,), (0,)), ((), ())), preferred_element_type=F32
        ).astype(BF16)
        for q in range(2):
            for h in range(4):
                for k in range(2):
                    row = h * 128 + k * 64
                    part = value[row : row + 64, q * COLS : q * COLS + COLS]
                    grad[j, k, 2 * p + q, h] = part

    def core_share(j, p):
        for q in (2 * p, 2 * p + 1):
            core_copies[j, q] = send(grad.at[j, 1 - c, q], core_in.at[j, q], core)

    def chip_sum(j, q):
        core_copies[j, q].wait_recv()
        for h in range(4):
            grad[j, c, q, h] = grad[j, c, q, h] + core_in[j, q, h]

    lo, hi = pl.ds(0, 2), pl.ds(2, 2)
    two, direct, fwd, y_copies, z_copies = {}, {}, {}, {}, {}
    far, mid0, mid1, last0, last1 = {}, {}, {}, {}, {}

    def send_two(q):
        two[q] = (
            send(grad.at[0, c, q, lo], two_in.at[q, 0], left),
            send(grad.at[0, c, q, hi], two_in.at[q, 1], right),
        )

    def send_right(q):
        direct[q, 0] = send(grad.at[1, c, q, lo], direct_in.at[q, 0], right)

    def send_left(q):
        direct[q, 1] = send(grad.at[2, c, q, hi], direct_in.at[q, 1], left)

    def forward(q):
        two[q][1].wait_recv()
        for h in range(2):
            grad[1, c, q, 2 + h] = grad[1, c, q, 2 + h] + two_in[q, 1, h]
        right_copy = send(grad.at[1, c, q, hi], fwd_in.at[q, 1], right)
        two[q][0].wait_recv()
        for h in range(2):
            grad[2, c, q, h] = grad[2, c, q, h] + two_in[q, 0, h]
        fwd[q] = (send(grad.at[2, c, q, lo], fwd_in.at[q, 0], left), right_copy)

    def finish_x(q):
        arrive(w_copies[q])
        arrive((direct[q, 0], direct[q, 1], *fwd[q]))
        for h in range(4):
            half, place = h // 2, h % 2
            total = grad[3, c, q, h].astype(F32) + direct_in[q, half, place].astype(F32)
            total = total + fwd_in[q, half, place].astype(F32)
            total = (total * weight[q, h].astype(F32)).astype(BF16)
            for t in range(4):
                y_own[q, t, h] = total[t * 16 : t * 16 + 16]
        y_copies[q] = [
            send(y_own.at[q, lax.rem(y + d, 4)], y_in.at[q, d - 1], shift("y", d)) for d in (2, 1, 3)
        ]

    def finish_y(q):
        arrive(y_copies[q])
        for h in range(4):
            total = y_own[q, y, h].astype(F32) + y_in[q, 0, h].astype(F32)
            total = total + y_in[q, 1, h].astype(F32) + y_in[q, 2, h].astype(F32)
            for s in range(2):
                z_own[q, h * 2 + s] = total[:, s * 128 : s * 128 + 128].astype(BF16)
        z_copies[q] = [
            send(z_own.at[q, lax.rem(z + d, 8)], z_in.at[q, d - 1], z_shift(d)) for d in FAR
        ]

    rows = pl.ds(pl.multiple_of(y * 16, 16), 16)

    def finish_z(q):
        arrive(z_copies[q])
        cut = pl.ds(pl.multiple_of(q * COLS + zl * 128, 128), 128)
        total = z_own[q, z].astype(F32)
        for d in range(7):
            total = total + z_in[q, d].astype(F32)
        pseudo = base_sum[zl, :, q * 128 : q * 128 + 128] / 8 + total
        fresh_m = inertia * mom[rows, cut] + pseudo
        fresh_p = outer[rows, cut] - outer_rate * (pseudo + inertia * fresh_m)
        cc[zh, x, c, rows, cut] = fresh_p.astype(BF16)
        nm[y, zl, :, q * 128 : q * 128 + 128] = fresh_m.astype(BF16)
        own = cc.at[zh, x, c, rows, cut]
        far[q] = [send(own, own, z_shift(d)) for d in FAR]

    def columns_of(q):
        return pl.ds(q * COLS, COLS)

    def gather_mid(q):
        arrive(far[q])
        part0 = cc.at[lo, x, c, rows, columns_of(q)]
        part1 = cc.at[hi, x, c, rows, columns_of(q)]
        mid0[q] = [send(part0, part0, shift("y", d)) for d in (2, 1, 3)]
        mid1[q] = [send(part1, part1, shift("x", d)) for d in (2, 1, 3)]

    def x_part(q, d, blocks=lo):
        return cc.at[blocks, lax.rem(x + d, 4), c, :, columns_of(q)]

    def y_part(q, d, blocks=hi):
        place = pl.ds(pl.multiple_of(lax.rem(y + d, 4) * 16, 16), 16)
        return cc.at[blocks, :, c, place, columns_of(q)]

    shared = []

    def core_send(part):
        shared.append(send(part, part, core))

    up, down = shift("y", 1), shift("y", 3)
    ring0, ring1, tails = {}, {}, {}

    def gather_last(q):
        arrive(mid0[q])
        part0 = x_part(q, 0)
        if q in DIRECT:
            last0[q] = [(d, send(part0, part0, shift("x", d))) for d in (2, 1, 3)]
        else:
            ring0[q] = [send(part0, part0, right), send(part0, part0, left)]
        arrive(mid1[q])
        part1 = y_part(q, 0)
        if q in DIRECT:
            last1[q] = [(d, send(part1, part1, shift("y", d))) for d in (2, 1, 3)]
            core_send(part0)
            core_send(part1)
        else:
            ring1[q] = [send(part1, part1, up), send(part1, part1, down)]

    def gather_on(q):
        def pass_on(copy, part, peer):
            copy.wait_recv()
            return send(part, part, peer)

        tails[q] = [
            pass_on(ring0[q][0], x_part(q, 3, pl.ds(0, 1)), right),
            pass_on(ring0[q][1], x_part(q, 1, pl.ds(1, 1)), left),
            pass_on(ring1[q][0], y_part(q, 3, pl.ds(2, 1)), up),
            pass_on(ring1[q][1], y_part(q, 1, pl.ds(3, 1)), down),
        ]

    def gather_core(q):
        if q not in DIRECT:
            arrive(tails[q])
            core_send(cc.at[:, :, c, :, columns_of(q)])
            return
        for i in (1, 2, 0):
            d, copy = last0[q][i]
            copy.wait_recv()
            core_send(x_part(q, 4 - d))
            d, copy = last1[q][i]
            copy.wait_recv()
            core_send(y_part(q, 4 - d))

    def share_weight(q):
        w_copies[q] = []
        for i, (d, half) in enumerate(((3, pl.ds(0, 32)), (1, pl.ds(32, 32)))):
            w_near[q][i].wait_recv()
            part = weight.at[q, lax.rem(zh + d, 4), half]
            w_copies[q].append(send(part, part, shift("zh", 4 - d)))

    zh_two, zh_direct, zh_fwd, zx_copies = [], [], [], []
    ahead, behind = shift("zh", 1), shift("zh", 3)

    def block(part, d):
        return grad.at[part, c, FIRST_Z, lax.rem(zh + d, 4)]

    def share_zh_two():
        zh_two.append(send(block(lo, 2), zh_two_in.at[0], behind))
        zh_two.append(send(block(hi, 2), zh_two_in.at[1], ahead))

    def share_zh_direct():
        zh_direct.append(send(block(lo, 1), zh_direct_in.at[0], ahead))
        zh_direct.append(send(block(hi, 3), zh_direct_in.at[1], behind))

    def forward_zh():
        for half, d, peer in ((0, 3, behind), (1, 1, ahead)):
            zh_two[half].wait_recv()
            there = lax.rem(zh + d, 4)
            for j in range(2):
                own = grad[2 * half + j, c, FIRST_Z, there]
                grad[2 * half + j, c, FIRST_Z, there] = own + zh_two_in[half, j]
            part = block((lo, hi)[half], d)
            zh_fwd.append(send(part, zh_fwd_in.at[half], peer))

    def sum_zh():
        arrive(zh_direct + zh_fwd)
        for j in range(4):
            half, place = j // 2, j % 2
            total = grad[j, c, FIRST_Z, zh].astype(F32) + zh_direct_in[half, place].astype(F32)
            zh_sum[j] = (total + zh_fwd_in[half, place].astype(F32)).astype(BF16)
            if j < 3:
                zx_copies.append(send(zh_sum.at[j], zx_in.at[j], shift("x", STEPS[j])))

    def sum_zx():
        arrive(zx_copies)
        total = zh_sum[3].astype(F32)
        for j in range(3):
            total = total + zx_in[j].astype(F32)
        total = (total * own_factor[...]).astype(BF16)
        for t in range(4):
            for s in range(2):
                rep_own[t, s] = total[t * 16 : t * 16 + 16, s * 128 : s * 128 + 128]
        z_copies[FIRST_Z] = []
        for dy, dz in ((2, 1), (1, 1), (3, 1), (2, 0), (1, 0), (3, 0), (0, 1)):
            peer = {**shift("y", dy), **shift("zl", dz)}
            part = rep_own.at[lax.rem(y + dy, 4), lax.rem(zl + dz, 2)]
            z_copies[FIRST_Z].append(send(part, z_in.at[FIRST_Z, 2 * dy + dz - 1], peer))
        z_own[FIRST_Z, z] = rep_own[y, zl]

    held = {}

    def base_pair():
        arrive(held["base_y"])
        base_sum[...] = base[y] + base_in[0] + base_in[1] + base_in[2]
        held["base"] = send(base_sum.at[1 - zl], base_far, pair)

    def base_total():
        held["base"].wait_recv()
        base_sum[zl] = base_sum[zl] + base_far[...]

    def make(*pairs):
        for j, p in pairs:
            product(j, p)
            core_share(j, p)

    product(0, 0)
    pl.semaphore_wait(barrier, len(peers))
    core_share(0, 0)
    moment_load.wait()
    factor = (inner_rate / (8 * 32768)) / (jnp.sqrt(moment[0]) + epsilon)
    for q in RING:
        weight[q, zh] = factor[:, q * COLS : q * COLS + COLS].astype(BF16)
    own_factor[...] = factor[:, FIRST_Z * COLS : FIRST_Z * COLS + COLS]
    w_near, w_copies = {}, {}
    for q in RING:
        part = weight.at[q, zh]
        w_near[q] = [send(part, part, shift("zh", d)) for d in (1, 3)]
    make((1, 0))
    chip_sum(0, 0)
    send_two(0)
    make((2, 0))
    chip_sum(1, 0)
    send_right(0)
    for copy in base_loads:
        copy.wait()
    for t in range(4):
        for s in range(2):
            for q in range(NQ):
                cols = slice(q * COLS + s * 128, q * COLS + s * 128 + 128)
                part = slice(t * 16, t * 16 + 16)
                base[t, s, :, q * 128 : q * 128 + 128] = outer[part, cols] - inner[0, part, cols]
    held["base_y"] = [
        send(base.at[lax.rem(y + d, 4)], base_in.at[d - 1], shift("y", d)) for d in (2, 1, 3)
    ]
    chip_sum(2, 0)
    send_left(0)
    make((0, 1), (1, 1))
    chip_sum(0, 2)
    send_two(2)
    make((3, 0))
    forward(0)
    share_weight(0)
    make((2, 1))
    for j in range(4):
        chip_sum(j, 1)
    share_zh_two()
    chip_sum(0, 3)
    send_two(3)
    chip_sum(1, 2)
    send_right(2)
    share_weight(2)
    share_weight(3)
    share_zh_direct()
    base_pair()
    chip_sum(2, 2)
    send_left(2)
    make((3, 1))
    forward(2)
    chip_sum(1, 3)
    send_right(3)
    chip_sum(2, 3)
    send_left(3)
    chip_sum(3, 0)
    mom_load.wait()

    def ready_sums():
        chip_sum(3, 2)
        chip_sum(3, 3)

    def fwd_and_next(q):
        forward(q)

    def nm_pair():
        part = nm.at[y, zl]
        held["nm"] = send(part, part, pair)

    def nm_y():
        held["nm"].wait_recv()
        part = nm.at[y]
        held["nm_y"] = [send(part, part, shift("y", d)) for d in (2, 1, 3)]

    stages = {
        "X": finish_x, "F": fwd_and_next, "Y": finish_y, "Z": finish_z, "M": gather_mid,
        "L": gather_last, "G": gather_on, "C": gather_core,
    }
    extra = {"cs": ready_sums, "zf": forward_zh, "zs": sum_zh, "zx": sum_zx, "bt": base_total, "np": nm_pair, "ny": nm_y}
    for name in ORDER:
        stage, operands = (extra[name], ()) if name in extra else (stages[name[0]], (int(name[1]),))
        stage(*operands)
    arrive(held["nm_y"])
    arrive(shared)
    for copy in sent:
        copy.wait_send()


def write(nm, cc, new_p, new_m, out, buf_p, buf_m, sem):
    zh, x, c = (lax.axis_index(a) for a in SHARD)
    copies = [pltpu.make_async_copy(cc.at[h], out.at[h], sem.at[h]) for h in range(4)]
    for copy in copies:
        copy.start()
    buf_p[...] = cc[zh, x, c].astype(F32)
    copies.append(pltpu.make_async_copy(buf_p, new_p, sem.at[4]))
    copies[4].start()
    for t in range(4):
        for s in range(2):
            for q in range(NQ):
                cols = slice(q * COLS + s * 128, q * COLS + s * 128 + 128)
                value = nm[t, s, :, q * 128 : q * 128 + 128].astype(F32)
                buf_m[t * 16 : t * 16 + 16, cols] = value
    copies.append(pltpu.make_async_copy(buf_m, new_m, sem.at[5]))
    copies[5].start()
    for copy in copies:
        copy.wait()


def per_device(activations, cotangents, inner_params, inner_moment, outer_params, momentum):
    vmem = pl.BlockSpec(memory_space=pltpu.VMEM)
    hbm = pl.BlockSpec(memory_space=pltpu.HBM)
    whole = (4, 4, 2, 64, 1024)
    nm, cc = pl.pallas_call(
        kernel,
        out_shape=(pltpu.VMEM((4, 2, 16, NQ * 128), BF16), pltpu.VMEM(whole, BF16)),
        in_specs=[hbm] * 6,
        out_specs=(vmem, vmem),
        scratch_shapes=[
            pltpu.VMEM((4, 1024, 512), BF16),
            pltpu.VMEM((2, 1024, 512), BF16),
            pltpu.VMEM((4, 2, NQ, 4, 64, COLS), BF16),
            pltpu.VMEM((4, NQ, 4, 64, COLS), BF16),
            pltpu.VMEM((NQ, 2, 2, 64, COLS), BF16),
            pltpu.VMEM((NQ, 2, 2, 64, COLS), BF16),
            pltpu.VMEM((NQ, 2, 2, 64, COLS), BF16),
            pltpu.VMEM((NQ, 4, 64, COLS), BF16),
            pltpu.VMEM((NQ, 4, 4, 16, COLS), BF16),
            pltpu.VMEM((NQ, 3, 4, 16, COLS), BF16),
            pltpu.VMEM((NQ, 8, 16, 128), BF16),
            pltpu.VMEM((NQ, 7, 16, 128), BF16),
            pltpu.VMEM((1, 64, 1024), F32),
            pltpu.VMEM((1, 64, 1024), F32),
            pltpu.VMEM((64, 1024), F32),
            pltpu.VMEM((64, 1024), F32),
            pltpu.VMEM((4, 2, 16, NQ * 128), F32),
            pltpu.VMEM((3, 2, 16, NQ * 128), F32),
            pltpu.VMEM((2, 16, NQ * 128), F32),
            pltpu.VMEM((16, NQ * 128), F32),
            pltpu.VMEM((64, COLS), F32),
            pltpu.VMEM((2, 2, 64, COLS), BF16),
            pltpu.VMEM((2, 2, 64, COLS), BF16),
            pltpu.VMEM((2, 2, 64, COLS), BF16),
            pltpu.VMEM((4, 64, COLS), BF16),
            pltpu.VMEM((3, 64, COLS), BF16),
            pltpu.VMEM((4, 2, 16, 128), BF16),
            pltpu.SemaphoreType.DMA((32,)),
            pltpu.SemaphoreType.DMA((SEMS,)),
            pltpu.SemaphoreType.DMA((SEMS,)),
        ],
        compiler_params=pltpu.CompilerParams(
            collective_id=0, has_side_effects=True, vmem_limit_bytes=61100 * 1024
        ),
    )(activations, cotangents, inner_params, inner_moment, outer_params, momentum)
    new_p, new_m, out = pl.pallas_call(
        write,
        out_shape=(
            jax.ShapeDtypeStruct((64, 1024), F32),
            jax.ShapeDtypeStruct((64, 1024), F32),
            jax.ShapeDtypeStruct(whole, BF16),
        ),
        in_specs=[vmem, vmem],
        out_specs=(hbm, hbm, hbm),
        scratch_shapes=[
            pltpu.VMEM((64, 1024), F32),
            pltpu.VMEM((64, 1024), F32),
            pltpu.SemaphoreType.DMA((6,)),
        ],
        compiler_params=pltpu.CompilerParams(vmem_limit_bytes=8 * 2**20),
    )(nm, cc)
    return new_p, new_m, out.reshape(2048, 1024)


def solution(mesh):
    split = Mesh(mesh.devices.reshape(*(SIZE[a] for a in AXES)), AXES)
    return jax.shard_map(
        per_device,
        mesh=split,
        in_specs=(
            P(AXES, None),
            P(AXES, None),
            P(REP, SHARD, None),
            P(REP, SHARD, None),
            P(SHARD, None),
            P(SHARD, None),
        ),
        out_specs=(P(SHARD, None), P(SHARD, None), P()),
        check_vma=False,
    )
```

```python
import functools

import jax
import jax.numpy as jnp
from jax import lax
from jax.experimental import pallas as pl
from jax.experimental.pallas import tpu as pltpu
from jax.sharding import Mesh
from jax.sharding import PartitionSpec as P

MESH = pl.DeviceIdType.MESH
AXES = ("zl", "y", "zh", "x", "c")
SIZE = {"zl": 2, "y": 4, "zh": 4, "x": 4, "c": 2}
REP = ("zl", "y")
SHARD = ("zh", "x", "c")
BF16, F32 = jnp.bfloat16, jnp.float32

outer_rate = 0.7
inertia = 0.9
inner_rate = 0.3
epsilon = 1e-08

NQ = 4
COLS = 1024 // NQ
RING = (0, 2, 3)
FIRST_Z = 1
ORDER = ("X0", "F3", "Y0", "cs", "zf", "X2", "X3", "Y2", "bt", "Z0", "Y3", "zs", "Z2", "M0", "zx", "Z3", "M2", "L0", "Z1", "np", "M3", "L2", "M1", "ny", "G0", "L3", "G2", "L1", "C0", "C3", "C2", "C1")
DIRECT = (1, 3)
SEMS = 200
STEPS = (2, 1, 3, 0)
FAR = (4, 3, 5, 2, 6, 1, 7)


def kernel(
    act, cot, inner_h, moment_h, outer_h, mom_h, nm, cc,
    a_buf, b_buf, grad, core_in, two_in, direct_in, fwd_in, weight, y_own, y_in, z_own, z_in,
    inner, moment, outer, mom, base, base_in, base_sum, base_far, own_factor, zh_two_in, zh_direct_in, zh_fwd_in, zh_sum, zx_in, rep_own, load_sem, ss, rs,
):
    zl, y, zh, x, c = (lax.axis_index(a) for a in AXES)
    at = {"zl": zl, "y": y, "zh": zh, "x": x, "c": c}

    def shift(axis, d):
        return {axis: lax.rem(at[axis] + d, SIZE[axis])}

    z = zh * 2 + zl

    def z_shift(d):
        there = lax.rem(z + d, 8)
        return {"zh": there // 2, "zl": lax.rem(there, 2)}

    core = {"c": 1 - c}
    pair = {"zl": 1 - zl}
    right, left = shift("x", 1), shift("x", 3)

    barrier = pltpu.get_barrier_semaphore()
    peers = [core, right, left] + [shift("y", d) for d in (1, 2, 3)]
    peers += [z_shift(d) for d in (1, 2, 6, 7)]
    for peer in peers:
        pl.semaphore_signal(barrier, inc=1, device_id=peer, device_id_type=MESH)

    loads = []

    def load(src, dst):
        copy = pltpu.make_async_copy(src, dst, load_sem.at[len(loads)])
        copy.start()
        loads.append(copy)

    a_loads, b_loads = {}, {}

    def load_a(j):
        there = lax.rem(x + STEPS[j], 4)
        for h in range(4):
            columns = pl.ds(pl.multiple_of(h * 512 + there * 128, 128), 128)
            load(act.at[:, columns], a_buf.at[j, :, pl.ds(h * 128, 128)])
        a_loads[j] = loads[-4:]

    def load_b(p):
        load(cot.at[:, pl.ds(p * 512, 512)], b_buf.at[p])
        b_loads[p] = loads[-1:]

    load_a(0)
    load_b(0)
    load(moment_h, moment)
    moment_load = loads[-1]
    load_a(1)
    load_a(2)
    load(inner_h, inner)
    load(outer_h, outer)
    base_loads = loads[-2:]
    load_a(3)
    load_b(1)
    load(mom_h, mom)
    mom_load = loads[-1]

    count = [0]
    sent = []

    def send(src, dst, peer):
        i = count[0]
        count[0] += 1
        copy = pltpu.make_async_remote_copy(
            src, dst, ss.at[i], rs.at[i], device_id=peer, device_id_type=MESH
        )
        copy.start()
        sent.append(copy)
        return copy

    def arrive(copies):
        for copy in copies:
            copy.wait_recv()

    core_copies = {}

    def product(j, p):
        for copy in a_loads.pop(j, []) + b_loads.pop(p, []):
            copy.wait()
        value = lax.dot_general(
            a_buf[j], b_buf[p], (((0,), (0,)), ((), ())), preferred_element_type=F32
        ).astype(BF16)
        for q in range(2):
            for h in range(4):
                for k in range(2):
                    row = h * 128 + k * 64
                    part = value[row : row + 64, q * COLS : q * COLS + COLS]
                    grad[j, k, 2 * p + q, h] = part

    def core_share(j, p, places=(0, 1)):
        for q in (2 * p + place for place in places):
            core_copies[j, q] = send(grad.at[j, 1 - c, q], core_in.at[j, q], core)

    def chip_sum(j, q):
        core_copies[j, q].wait_recv()
        for h in range(4):
            grad[j, c, q, h] = grad[j, c, q, h] + core_in[j, q, h]

    lo, hi = pl.ds(0, 2), pl.ds(2, 2)
    two, direct, fwd, y_copies, z_copies = {}, {}, {}, {}, {}
    far, mid0, mid1, last0, last1 = {}, {}, {}, {}, {}

    def send_two(q):
        two[q] = (
            send(grad.at[0, c, q, lo], two_in.at[q, 0], left),
            send(grad.at[0, c, q, hi], two_in.at[q, 1], right),
        )

    def send_right(q):
        direct[q, 0] = send(grad.at[1, c, q, lo], direct_in.at[q, 0], right)

    def send_left(q):
        direct[q, 1] = send(grad.at[2, c, q, hi], direct_in.at[q, 1], left)

    def forward(q):
        two[q][1].wait_recv()
        for h in range(2):
            grad[1, c, q, 2 + h] = grad[1, c, q, 2 + h] + two_in[q, 1, h]
        right_copy = send(grad.at[1, c, q, hi], fwd_in.at[q, 1], right)
        two[q][0].wait_recv()
        for h in range(2):
            grad[2, c, q, h] = grad[2, c, q, h] + two_in[q, 0, h]
        fwd[q] = (send(grad.at[2, c, q, lo], fwd_in.at[q, 0], left), right_copy)

    def finish_x(q):
        arrive(w_copies[q])
        arrive((direct[q, 0], direct[q, 1], *fwd[q]))
        for h in range(4):
            half, place = h // 2, h % 2
            total = grad[3, c, q, h].astype(F32) + direct_in[q, half, place].astype(F32)
            total = total + fwd_in[q, half, place].astype(F32)
            total = (total * weight[q, h].astype(F32)).astype(BF16)
            for t in range(4):
                y_own[q, t, h] = total[t * 16 : t * 16 + 16]
        y_copies[q] = [
            send(y_own.at[q, lax.rem(y + d, 4)], y_in.at[q, d - 1], shift("y", d)) for d in (2, 1, 3)
        ]

    def finish_y(q):
        arrive(y_copies[q])
        for h in range(4):
            total = y_own[q, y, h].astype(F32) + y_in[q, 0, h].astype(F32)
            total = total + y_in[q, 1, h].astype(F32) + y_in[q, 2, h].astype(F32)
            for s in range(2):
                z_own[q, h * 2 + s] = total[:, s * 128 : s * 128 + 128].astype(BF16)
        z_copies[q] = [
            send(z_own.at[q, lax.rem(z + d, 8)], z_in.at[q, d - 1], z_shift(d)) for d in FAR
        ]

    rows = pl.ds(pl.multiple_of(y * 16, 16), 16)

    def finish_z(q):
        arrive(z_copies[q])
        cut = pl.ds(pl.multiple_of(q * COLS + zl * 128, 128), 128)
        total = z_own[q, z].astype(F32)
        for d in range(7):
            total = total + z_in[q, d].astype(F32)
        pseudo = base_sum[zl, :, q * 128 : q * 128 + 128] / 8 + total
        fresh_m = inertia * mom[rows, cut] + pseudo
        fresh_p = outer[rows, cut] - outer_rate * (pseudo + inertia * fresh_m)
        cc[zh, x, c, rows, cut] = fresh_p.astype(BF16)
        nm[y, zl, :, q * 128 : q * 128 + 128] = fresh_m.astype(BF16)
        own = cc.at[zh, x, c, rows, cut]
        far[q] = [send(own, own, z_shift(d)) for d in FAR]

    def columns_of(q):
        return pl.ds(q * COLS, COLS)

    def gather_mid(q):
        arrive(far[q])
        part0 = cc.at[lo, x, c, rows, columns_of(q)]
        part1 = cc.at[hi, x, c, rows, columns_of(q)]
        mid0[q] = [send(part0, part0, shift("y", d)) for d in (2, 1, 3)]
        mid1[q] = [send(part1, part1, shift("x", d)) for d in (2, 1, 3)]

    def x_part(q, d, blocks=lo):
        return cc.at[blocks, lax.rem(x + d, 4), c, :, columns_of(q)]

    def y_part(q, d, blocks=hi):
        place = pl.ds(pl.multiple_of(lax.rem(y + d, 4) * 16, 16), 16)
        return cc.at[blocks, :, c, place, columns_of(q)]

    shared = []

    def core_send(part):
        shared.append(send(part, part, core))

    up, down = shift("y", 1), shift("y", 3)
    ring0, ring1, tails = {}, {}, {}

    def gather_last(q):
        arrive(mid0[q])
        part0 = x_part(q, 0)
        if q in DIRECT:
            last0[q] = [(d, send(part0, part0, shift("x", d))) for d in (2, 1, 3)]
        else:
            ring0[q] = [send(part0, part0, right), send(part0, part0, left)]
        arrive(mid1[q])
        part1 = y_part(q, 0)
        if q in DIRECT:
            last1[q] = [(d, send(part1, part1, shift("y", d))) for d in (2, 1, 3)]
            core_send(part0)
            core_send(part1)
        else:
            ring1[q] = [send(part1, part1, up), send(part1, part1, down)]

    def gather_on(q):
        def pass_on(copy, part, peer):
            copy.wait_recv()
            return send(part, part, peer)

        tails[q] = [
            pass_on(ring0[q][0], x_part(q, 3, pl.ds(0, 1)), right),
            pass_on(ring0[q][1], x_part(q, 1, pl.ds(1, 1)), left),
            pass_on(ring1[q][0], y_part(q, 3, pl.ds(2, 1)), up),
            pass_on(ring1[q][1], y_part(q, 1, pl.ds(3, 1)), down),
        ]

    def gather_core(q):
        if q not in DIRECT:
            arrive(tails[q])
            core_send(cc.at[:, :, c, :, columns_of(q)])
            return
        for i in (1, 2, 0):
            d, copy = last0[q][i]
            copy.wait_recv()
            core_send(x_part(q, 4 - d))
            d, copy = last1[q][i]
            copy.wait_recv()
            core_send(y_part(q, 4 - d))

    def share_weight(q):
        w_copies[q] = []
        for i, (d, half) in enumerate(((3, pl.ds(0, 32)), (1, pl.ds(32, 32)))):
            w_near[q][i].wait_recv()
            part = weight.at[q, lax.rem(zh + d, 4), half]
            w_copies[q].append(send(part, part, shift("zh", 4 - d)))

    zh_two, zh_direct, zh_fwd, zx_copies = [], [], [], []
    ahead, behind = shift("zh", 1), shift("zh", 3)

    def block(part, d):
        return grad.at[part, c, FIRST_Z, lax.rem(zh + d, 4)]

    def share_zh_two():
        zh_two.append(send(block(lo, 2), zh_two_in.at[0], behind))
        zh_two.append(send(block(hi, 2), zh_two_in.at[1], ahead))

    def share_zh_direct():
        zh_direct.append(send(block(lo, 1), zh_direct_in.at[0], ahead))
        zh_direct.append(send(block(hi, 3), zh_direct_in.at[1], behind))

    def forward_zh():
        for half, d, peer in ((0, 3, behind), (1, 1, ahead)):
            zh_two[half].wait_recv()
            there = lax.rem(zh + d, 4)
            for j in range(2):
                own = grad[2 * half + j, c, FIRST_Z, there]
                grad[2 * half + j, c, FIRST_Z, there] = own + zh_two_in[half, j]
            part = block((lo, hi)[half], d)
            zh_fwd.append(send(part, zh_fwd_in.at[half], peer))

    def sum_zh():
        arrive(zh_direct + zh_fwd)
        for j in range(4):
            half, place = j // 2, j % 2
            total = grad[j, c, FIRST_Z, zh].astype(F32) + zh_direct_in[half, place].astype(F32)
            zh_sum[j] = (total + zh_fwd_in[half, place].astype(F32)).astype(BF16)
            if j < 3:
                zx_copies.append(send(zh_sum.at[j], zx_in.at[j], shift("x", STEPS[j])))

    def sum_zx():
        arrive(zx_copies)
        total = zh_sum[3].astype(F32)
        for j in range(3):
            total = total + zx_in[j].astype(F32)
        total = (total * own_factor[...]).astype(BF16)
        for t in range(4):
            for s in range(2):
                rep_own[t, s] = total[t * 16 : t * 16 + 16, s * 128 : s * 128 + 128]
        z_copies[FIRST_Z] = []
        for dy, dz in ((2, 1), (1, 1), (3, 1), (2, 0), (1, 0), (3, 0), (0, 1)):
            peer = {**shift("y", dy), **shift("zl", dz)}
            part = rep_own.at[lax.rem(y + dy, 4), lax.rem(zl + dz, 2)]
            z_copies[FIRST_Z].append(send(part, z_in.at[FIRST_Z, 2 * dy + dz - 1], peer))
        z_own[FIRST_Z, z] = rep_own[y, zl]

    held = {}

    def base_pair():
        arrive(held["base_y"])
        base_sum[...] = base[y] + base_in[0] + base_in[1] + base_in[2]
        held["base"] = send(base_sum.at[1 - zl], base_far, pair)

    def base_total():
        held["base"].wait_recv()
        base_sum[zl] = base_sum[zl] + base_far[...]

    def make(*pairs):
        for j, p in pairs:
            product(j, p)
            core_share(j, p)

    product(0, 0)
    pl.semaphore_wait(barrier, len(peers))
    core_share(0, 0, (0,))
    moment_load.wait()
    factor = (inner_rate / (8 * 32768)) / (jnp.sqrt(moment[0]) + epsilon)
    for q in RING:
        weight[q, zh] = factor[:, q * COLS : q * COLS + COLS].astype(BF16)
    own_factor[...] = factor[:, FIRST_Z * COLS : FIRST_Z * COLS + COLS]
    w_near, w_copies = {}, {}
    for q in RING:
        part = weight.at[q, zh]
        w_near[q] = [send(part, part, shift("zh", d)) for d in (1, 3)]
    make((1, 0))
    chip_sum(0, 0)
    send_two(0)
    core_share(0, 0, (1,))
    make((2, 0))
    chip_sum(1, 0)
    send_right(0)
    for copy in base_loads:
        copy.wait()
    for t in range(4):
        for s in range(2):
            for q in range(NQ):
                cols = slice(q * COLS + s * 128, q * COLS + s * 128 + 128)
                part = slice(t * 16, t * 16 + 16)
                base[t, s, :, q * 128 : q * 128 + 128] = outer[part, cols] - inner[0, part, cols]
    held["base_y"] = [
        send(base.at[lax.rem(y + d, 4)], base_in.at[d - 1], shift("y", d)) for d in (2, 1, 3)
    ]
    chip_sum(2, 0)
    send_left(0)
    make((0, 1), (1, 1))
    chip_sum(0, 2)
    send_two(2)
    make((3, 0))
    forward(0)
    share_weight(0)
    make((2, 1))
    for j in range(4):
        chip_sum(j, 1)
    share_zh_two()
    chip_sum(0, 3)
    send_two(3)
    chip_sum(1, 2)
    send_right(2)
    share_weight(2)
    share_weight(3)
    share_zh_direct()
    base_pair()
    chip_sum(2, 2)
    send_left(2)
    make((3, 1))
    forward(2)
    chip_sum(1, 3)
    send_right(3)
    chip_sum(2, 3)
    send_left(3)
    chip_sum(3, 0)
    mom_load.wait()

    def ready_sums():
        chip_sum(3, 2)
        chip_sum(3, 3)

    def fwd_and_next(q):
        forward(q)

    def nm_pair():
        part = nm.at[y, zl]
        held["nm"] = send(part, part, pair)

    def nm_y():
        held["nm"].wait_recv()
        part = nm.at[y]
        held["nm_y"] = [send(part, part, shift("y", d)) for d in (2, 1, 3)]

    stages = {
        "X": finish_x, "F": fwd_and_next, "Y": finish_y, "Z": finish_z, "M": gather_mid,
        "L": gather_last, "G": gather_on, "C": gather_core,
    }
    extra = {"cs": ready_sums, "zf": forward_zh, "zs": sum_zh, "zx": sum_zx, "bt": base_total, "np": nm_pair, "ny": nm_y}
    for name in ORDER:
        stage, operands = (extra[name], ()) if name in extra else (stages[name[0]], (int(name[1]),))
        stage(*operands)
    arrive(held["nm_y"])
    arrive(shared)
    for copy in sent:
        copy.wait_send()


def write(nm, cc, new_p, new_m, out, buf_p, buf_m, sem):
    zh, x, c = (lax.axis_index(a) for a in SHARD)
    copies = [pltpu.make_async_copy(cc.at[h], out.at[h], sem.at[h]) for h in range(4)]
    for copy in copies:
        copy.start()
    buf_p[...] = cc[zh, x, c].astype(F32)
    copies.append(pltpu.make_async_copy(buf_p, new_p, sem.at[4]))
    copies[4].start()
    for t in range(4):
        for s in range(2):
            for q in range(NQ):
                cols = slice(q * COLS + s * 128, q * COLS + s * 128 + 128)
                value = nm[t, s, :, q * 128 : q * 128 + 128].astype(F32)
                buf_m[t * 16 : t * 16 + 16, cols] = value
    copies.append(pltpu.make_async_copy(buf_m, new_m, sem.at[5]))
    copies[5].start()
    for copy in copies:
        copy.wait()


def per_device(activations, cotangents, inner_params, inner_moment, outer_params, momentum):
    vmem = pl.BlockSpec(memory_space=pltpu.VMEM)
    hbm = pl.BlockSpec(memory_space=pltpu.HBM)
    whole = (4, 4, 2, 64, 1024)
    nm, cc = pl.pallas_call(
        kernel,
        out_shape=(pltpu.VMEM((4, 2, 16, NQ * 128), BF16), pltpu.VMEM(whole, BF16)),
        in_specs=[hbm] * 6,
        out_specs=(vmem, vmem),
        scratch_shapes=[
            pltpu.VMEM((4, 1024, 512), BF16),
            pltpu.VMEM((2, 1024, 512), BF16),
            pltpu.VMEM((4, 2, NQ, 4, 64, COLS), BF16),
            pltpu.VMEM((4, NQ, 4, 64, COLS), BF16),
            pltpu.VMEM((NQ, 2, 2, 64, COLS), BF16),
            pltpu.VMEM((NQ, 2, 2, 64, COLS), BF16),
            pltpu.VMEM((NQ, 2, 2, 64, COLS), BF16),
            pltpu.VMEM((NQ, 4, 64, COLS), BF16),
            pltpu.VMEM((NQ, 4, 4, 16, COLS), BF16),
            pltpu.VMEM((NQ, 3, 4, 16, COLS), BF16),
            pltpu.VMEM((NQ, 8, 16, 128), BF16),
            pltpu.VMEM((NQ, 7, 16, 128), BF16),
            pltpu.VMEM((1, 64, 1024), F32),
            pltpu.VMEM((1, 64, 1024), F32),
            pltpu.VMEM((64, 1024), F32),
            pltpu.VMEM((64, 1024), F32),
            pltpu.VMEM((4, 2, 16, NQ * 128), F32),
            pltpu.VMEM((3, 2, 16, NQ * 128), F32),
            pltpu.VMEM((2, 16, NQ * 128), F32),
            pltpu.VMEM((16, NQ * 128), F32),
            pltpu.VMEM((64, COLS), F32),
            pltpu.VMEM((2, 2, 64, COLS), BF16),
            pltpu.VMEM((2, 2, 64, COLS), BF16),
            pltpu.VMEM((2, 2, 64, COLS), BF16),
            pltpu.VMEM((4, 64, COLS), BF16),
            pltpu.VMEM((3, 64, COLS), BF16),
            pltpu.VMEM((4, 2, 16, 128), BF16),
            pltpu.SemaphoreType.DMA((32,)),
            pltpu.SemaphoreType.DMA((SEMS,)),
            pltpu.SemaphoreType.DMA((SEMS,)),
        ],
        compiler_params=pltpu.CompilerParams(
            collective_id=0, has_side_effects=True, vmem_limit_bytes=61100 * 1024
        ),
    )(activations, cotangents, inner_params, inner_moment, outer_params, momentum)
    new_p, new_m, out = pl.pallas_call(
        write,
        out_shape=(
            jax.ShapeDtypeStruct((64, 1024), F32),
            jax.ShapeDtypeStruct((64, 1024), F32),
            jax.ShapeDtypeStruct(whole, BF16),
        ),
        in_specs=[vmem, vmem],
        out_specs=(hbm, hbm, hbm),
        scratch_shapes=[
            pltpu.VMEM((64, 1024), F32),
            pltpu.VMEM((64, 1024), F32),
            pltpu.SemaphoreType.DMA((6,)),
        ],
        compiler_params=pltpu.CompilerParams(vmem_limit_bytes=8 * 2**20),
    )(nm, cc)
    return new_p, new_m, out.reshape(2048, 1024)


def solution(mesh):
    split = Mesh(mesh.devices.reshape(*(SIZE[a] for a in AXES)), AXES)
    return jax.shard_map(
        per_device,
        mesh=split,
        in_specs=(
            P(AXES, None),
            P(AXES, None),
            P(REP, SHARD, None),
            P(REP, SHARD, None),
            P(SHARD, None),
            P(SHARD, None),
        ),
        out_specs=(P(SHARD, None), P(SHARD, None), P()),
        check_vma=False,
    )
```

```python
import functools

import jax
import jax.numpy as jnp
from jax import lax
from jax.experimental import pallas as pl
from jax.experimental.pallas import tpu as pltpu
from jax.sharding import Mesh
from jax.sharding import PartitionSpec as P

MESH = pl.DeviceIdType.MESH
AXES = ("zl", "y", "zh", "x", "c")
SIZE = {"zl": 2, "y": 4, "zh": 4, "x": 4, "c": 2}
REP = ("zl", "y")
SHARD = ("zh", "x", "c")
BF16, F32 = jnp.bfloat16, jnp.float32

outer_rate = 0.7
inertia = 0.9
inner_rate = 0.3
epsilon = 1e-08

NQ = 4
COLS = 1024 // NQ
RING = (0, 2, 3)
FIRST_Z = 1
ORDER = ("X0", "F3", "Y0", "cs", "zf", "X2", "X3", "Y2", "bt", "Z0", "Y3", "zs", "Z2", "M0", "zx", "Z3", "M2", "L0", "Z1", "np", "M3", "L2", "M1", "ny", "G0", "L3", "G2", "L1", "C0", "C3", "C2", "C1")
DIRECT = (1, 3)
SEMS = 200
STEPS = (2, 1, 3, 0)
FAR = (4, 3, 5, 2, 6, 1, 7)


def kernel(
    act, cot, inner_h, moment_h, outer_h, mom_h, nm, cc,
    a_buf, b_buf, grad, core_in, two_in, direct_in, fwd_in, weight, y_own, y_in, z_own, z_in,
    inner, moment, outer, mom, base, base_in, base_sum, base_far, own_factor, zh_two_in, zh_direct_in, zh_fwd_in, zh_sum, zx_in, rep_own, load_sem, ss, rs,
):
    zl, y, zh, x, c = (lax.axis_index(a) for a in AXES)
    at = {"zl": zl, "y": y, "zh": zh, "x": x, "c": c}

    def shift(axis, d):
        return {axis: lax.rem(at[axis] + d, SIZE[axis])}

    z = zh * 2 + zl

    def z_shift(d):
        there = lax.rem(z + d, 8)
        return {"zh": there // 2, "zl": lax.rem(there, 2)}

    core = {"c": 1 - c}
    pair = {"zl": 1 - zl}
    right, left = shift("x", 1), shift("x", 3)

    barrier = pltpu.get_barrier_semaphore()
    peers = [core, right, left] + [shift("y", d) for d in (1, 2, 3)]
    peers += [z_shift(d) for d in (1, 2, 6, 7)]
    for peer in peers:
        pl.semaphore_signal(barrier, inc=1, device_id=peer, device_id_type=MESH)

    loads = []

    def load(src, dst):
        copy = pltpu.make_async_copy(src, dst, load_sem.at[len(loads)])
        copy.start()
        loads.append(copy)

    a_loads, b_loads = {}, {}

    def load_a(j):
        there = lax.rem(x + STEPS[j], 4)
        for h in range(4):
            columns = pl.ds(pl.multiple_of(h * 512 + there * 128, 128), 128)
            load(act.at[:, columns], a_buf.at[j, :, pl.ds(h * 128, 128)])
        a_loads[j] = loads[-4:]

    def load_b(p):
        load(cot.at[:, pl.ds(p * 512, 512)], b_buf.at[p])
        b_loads[p] = loads[-1:]

    load_a(0)
    load_b(0)
    load(moment_h, moment)
    moment_load = loads[-1]
    load_a(1)
    load_a(2)
    load(inner_h, inner)
    load(outer_h, outer)
    base_loads = loads[-2:]
    load_a(3)
    load_b(1)
    load(mom_h, mom)
    mom_load = loads[-1]

    count = [0]
    sent = []

    def send(src, dst, peer):
        i = count[0]
        count[0] += 1
        copy = pltpu.make_async_remote_copy(
            src, dst, ss.at[i], rs.at[i], device_id=peer, device_id_type=MESH
        )
        copy.start()
        sent.append(copy)
        return copy

    def arrive(copies):
        for copy in copies:
            copy.wait_recv()

    core_copies = {}

    def product(j, p):
        for copy in a_loads.pop(j, []) + b_loads.pop(p, []):
            copy.wait()
        value = lax.dot_general(
            a_buf[j], b_buf[p], (((0,), (0,)), ((), ())), preferred_element_type=F32
        ).astype(BF16)
        for q in range(2):
            for h in range(4):
                for k in range(2):
                    row = h * 128 + k * 64
                    part = value[row : row + 64, q * COLS : q * COLS + COLS]
                    grad[j, k, 2 * p + q, h] = part

    def core_share(j, p, places=(0, 1)):
        for q in (2 * p + place for place in places):
            core_copies[j, q] = send(grad.at[j, 1 - c, q], core_in.at[j, q], core)

    def chip_sum(j, q):
        core_copies[j, q].wait_recv()
        for h in range(4):
            grad[j, c, q, h] = grad[j, c, q, h] + core_in[j, q, h]

    lo, hi = pl.ds(0, 2), pl.ds(2, 2)
    two, direct, fwd, y_copies, z_copies = {}, {}, {}, {}, {}
    far, mid0, mid1, last0, last1 = {}, {}, {}, {}, {}

    def send_two(q):
        two[q] = (
            send(grad.at[0, c, q, lo], two_in.at[q, 0], left),
            send(grad.at[0, c, q, hi], two_in.at[q, 1], right),
        )

    def send_right(q):
        direct[q, 0] = send(grad.at[1, c, q, lo], direct_in.at[q, 0], right)

    def send_left(q):
        direct[q, 1] = send(grad.at[2, c, q, hi], direct_in.at[q, 1], left)

    def forward(q):
        two[q][1].wait_recv()
        for h in range(2):
            grad[1, c, q, 2 + h] = grad[1, c, q, 2 + h] + two_in[q, 1, h]
        right_copy = send(grad.at[1, c, q, hi], fwd_in.at[q, 1], right)
        two[q][0].wait_recv()
        for h in range(2):
            grad[2, c, q, h] = grad[2, c, q, h] + two_in[q, 0, h]
        fwd[q] = (send(grad.at[2, c, q, lo], fwd_in.at[q, 0], left), right_copy)

    def finish_x(q):
        arrive(w_copies[q])
        arrive((direct[q, 0], direct[q, 1], *fwd[q]))
        for h in range(4):
            half, place = h // 2, h % 2
            total = grad[3, c, q, h].astype(F32) + direct_in[q, half, place].astype(F32)
            total = total + fwd_in[q, half, place].astype(F32)
            total = (total * weight[q, h].astype(F32)).astype(BF16)
            for t in range(4):
                y_own[q, t, h] = total[t * 16 : t * 16 + 16]
        y_copies[q] = [
            send(y_own.at[q, lax.rem(y + d, 4)], y_in.at[q, d - 1], shift("y", d)) for d in (2, 1, 3)
        ]

    def finish_y(q):
        arrive(y_copies[q])
        for h in range(4):
            total = y_own[q, y, h].astype(F32) + y_in[q, 0, h].astype(F32)
            total = total + y_in[q, 1, h].astype(F32) + y_in[q, 2, h].astype(F32)
            for s in range(2):
                z_own[q, h * 2 + s] = total[:, s * 128 : s * 128 + 128].astype(BF16)
        z_copies[q] = [
            send(z_own.at[q, lax.rem(z + d, 8)], z_in.at[q, d - 1], z_shift(d)) for d in FAR
        ]

    rows = pl.ds(pl.multiple_of(y * 16, 16), 16)

    def finish_z(q):
        arrive(z_copies[q])
        cut = pl.ds(pl.multiple_of(q * COLS + zl * 128, 128), 128)
        total = z_own[q, z].astype(F32)
        for d in range(7):
            total = total + z_in[q, d].astype(F32)
        pseudo = base_sum[zl, :, q * 128 : q * 128 + 128] / 8 + total
        fresh_m = inertia * mom[rows, cut] + pseudo
        fresh_p = outer[rows, cut] - outer_rate * (pseudo + inertia * fresh_m)
        cc[zh, x, c, rows, cut] = fresh_p.astype(BF16)
        nm[y, zl, :, q * 128 : q * 128 + 128] = fresh_m.astype(BF16)
        own = cc.at[zh, x, c, rows, cut]
        far[q] = [send(own, own, z_shift(d)) for d in FAR]

    def columns_of(q):
        return pl.ds(q * COLS, COLS)

    def gather_mid(q):
        arrive(far[q])
        part0 = cc.at[lo, x, c, rows, columns_of(q)]
        part1 = cc.at[hi, x, c, rows, columns_of(q)]
        mid0[q] = [send(part0, part0, shift("y", d)) for d in (2, 1, 3)]
        mid1[q] = [send(part1, part1, shift("x", d)) for d in (2, 1, 3)]

    def x_part(q, d, blocks=lo):
        return cc.at[blocks, lax.rem(x + d, 4), c, :, columns_of(q)]

    def y_part(q, d, blocks=hi):
        place = pl.ds(pl.multiple_of(lax.rem(y + d, 4) * 16, 16), 16)
        return cc.at[blocks, :, c, place, columns_of(q)]

    shared = []

    def core_send(part):
        shared.append(send(part, part, core))

    up, down = shift("y", 1), shift("y", 3)
    ring0, ring1, tails = {}, {}, {}

    def gather_last(q):
        arrive(mid0[q])
        part0 = x_part(q, 0)
        if q in DIRECT:
            last0[q] = [(d, send(part0, part0, shift("x", d))) for d in (2, 1, 3)]
        else:
            ring0[q] = [send(part0, part0, right), send(part0, part0, left)]
        arrive(mid1[q])
        part1 = y_part(q, 0)
        if q in DIRECT:
            last1[q] = [(d, send(part1, part1, shift("y", d))) for d in (2, 1, 3)]
            core_send(part0)
            core_send(part1)
        else:
            ring1[q] = [send(part1, part1, up), send(part1, part1, down)]

    def gather_on(q):
        def pass_on(copy, part, peer):
            copy.wait_recv()
            return send(part, part, peer)

        tails[q] = [
            pass_on(ring0[q][0], x_part(q, 3, pl.ds(0, 1)), right),
            pass_on(ring0[q][1], x_part(q, 1, pl.ds(1, 1)), left),
            pass_on(ring1[q][0], y_part(q, 3, pl.ds(2, 1)), up),
            pass_on(ring1[q][1], y_part(q, 1, pl.ds(3, 1)), down),
        ]

    def gather_core(q):
        if q not in DIRECT:
            arrive(tails[q])
            core_send(cc.at[:, :, c, :, columns_of(q)])
            return
        for i in (1, 2, 0):
            d, copy = last0[q][i]
            copy.wait_recv()
            core_send(x_part(q, 4 - d))
            d, copy = last1[q][i]
            copy.wait_recv()
            core_send(y_part(q, 4 - d))

    def share_weight(q):
        w_copies[q] = []
        for i, (d, half) in enumerate(((3, pl.ds(0, 32)), (1, pl.ds(32, 32)))):
            w_near[q][i].wait_recv()
            part = weight.at[q, lax.rem(zh + d, 4), half]
            w_copies[q].append(send(part, part, shift("zh", 4 - d)))

    zh_two, zh_direct, zh_fwd, zx_copies = [], [], [], []
    ahead, behind = shift("zh", 1), shift("zh", 3)

    def block(part, d):
        return grad.at[part, c, FIRST_Z, lax.rem(zh + d, 4)]

    def share_zh_two():
        zh_two.append(send(block(lo, 2), zh_two_in.at[0], behind))
        zh_two.append(send(block(hi, 2), zh_two_in.at[1], ahead))

    def share_zh_direct():
        zh_direct.append(send(block(lo, 1), zh_direct_in.at[0], ahead))
        zh_direct.append(send(block(hi, 3), zh_direct_in.at[1], behind))

    def forward_zh():
        for half, d, peer in ((0, 3, behind), (1, 1, ahead)):
            zh_two[half].wait_recv()
            there = lax.rem(zh + d, 4)
            for j in range(2):
                own = grad[2 * half + j, c, FIRST_Z, there]
                grad[2 * half + j, c, FIRST_Z, there] = own + zh_two_in[half, j]
            part = block((lo, hi)[half], d)
            zh_fwd.append(send(part, zh_fwd_in.at[half], peer))

    def sum_zh():
        arrive(zh_direct + zh_fwd)
        for j in range(4):
            half, place = j // 2, j % 2
            total = grad[j, c, FIRST_Z, zh].astype(F32) + zh_direct_in[half, place].astype(F32)
            zh_sum[j] = (total + zh_fwd_in[half, place].astype(F32)).astype(BF16)
            if j < 3:
                zx_copies.append(send(zh_sum.at[j], zx_in.at[j], shift("x", STEPS[j])))

    def sum_zx():
        arrive(zx_copies)
        total = zh_sum[3].astype(F32)
        for j in range(3):
            total = total + zx_in[j].astype(F32)
        total = (total * own_factor[...]).astype(BF16)
        for t in range(4):
            for s in range(2):
                rep_own[t, s] = total[t * 16 : t * 16 + 16, s * 128 : s * 128 + 128]
        z_copies[FIRST_Z] = []
        for dy, dz in ((2, 1), (1, 1), (3, 1), (2, 0), (1, 0), (3, 0), (0, 1)):
            peer = {**shift("y", dy), **shift("zl", dz)}
            part = rep_own.at[lax.rem(y + dy, 4), lax.rem(zl + dz, 2)]
            z_copies[FIRST_Z].append(send(part, z_in.at[FIRST_Z, 2 * dy + dz - 1], peer))
        z_own[FIRST_Z, z] = rep_own[y, zl]

    held = {}

    def base_pair():
        arrive(held["base_y"])
        base_sum[...] = base[y] + base_in[0] + base_in[1] + base_in[2]
        held["base"] = send(base_sum.at[1 - zl], base_far, pair)

    def base_total():
        held["base"].wait_recv()
        base_sum[zl] = base_sum[zl] + base_far[...]

    def make(*pairs):
        for j, p in pairs:
            product(j, p)
            core_share(j, p)

    product(0, 0)
    pl.semaphore_wait(barrier, len(peers))
    core_share(0, 0, (0,))
    moment_load.wait()
    factor = (inner_rate / (8 * 32768)) / (jnp.sqrt(moment[0]) + epsilon)
    for q in RING:
        weight[q, zh] = factor[:, q * COLS : q * COLS + COLS].astype(BF16)
    own_factor[...] = factor[:, FIRST_Z * COLS : FIRST_Z * COLS + COLS]
    w_near, w_copies = {}, {}

    def start_weight(q):
        part = weight.at[q, zh]
        w_near[q] = [send(part, part, shift("zh", d)) for d in (1, 3)]

    start_weight(0)
    make((1, 0))
    chip_sum(0, 0)
    send_two(0)
    core_share(0, 0, (1,))
    for q in (2, 3):
        start_weight(q)
    make((2, 0))
    chip_sum(1, 0)
    send_right(0)
    for copy in base_loads:
        copy.wait()
    for t in range(4):
        for s in range(2):
            for q in range(NQ):
                cols = slice(q * COLS + s * 128, q * COLS + s * 128 + 128)
                part = slice(t * 16, t * 16 + 16)
                base[t, s, :, q * 128 : q * 128 + 128] = outer[part, cols] - inner[0, part, cols]
    held["base_y"] = [
        send(base.at[lax.rem(y + d, 4)], base_in.at[d - 1], shift("y", d)) for d in (2, 1, 3)
    ]
    chip_sum(2, 0)
    send_left(0)
    make((0, 1), (1, 1))
    chip_sum(0, 2)
    send_two(2)
    make((3, 0))
    forward(0)
    share_weight(0)
    make((2, 1))
    for j in range(4):
        chip_sum(j, 1)
    share_zh_two()
    chip_sum(0, 3)
    send_two(3)
    chip_sum(1, 2)
    send_right(2)
    share_weight(2)
    share_weight(3)
    share_zh_direct()
    base_pair()
    chip_sum(2, 2)
    send_left(2)
    make((3, 1))
    forward(2)
    chip_sum(1, 3)
    send_right(3)
    chip_sum(2, 3)
    send_left(3)
    chip_sum(3, 0)
    mom_load.wait()

    def ready_sums():
        chip_sum(3, 2)
        chip_sum(3, 3)

    def fwd_and_next(q):
        forward(q)

    def nm_pair():
        part = nm.at[y, zl]
        held["nm"] = send(part, part, pair)

    def nm_y():
        held["nm"].wait_recv()
        part = nm.at[y]
        held["nm_y"] = [send(part, part, shift("y", d)) for d in (2, 1, 3)]

    stages = {
        "X": finish_x, "F": fwd_and_next, "Y": finish_y, "Z": finish_z, "M": gather_mid,
        "L": gather_last, "G": gather_on, "C": gather_core,
    }
    extra = {"cs": ready_sums, "zf": forward_zh, "zs": sum_zh, "zx": sum_zx, "bt": base_total, "np": nm_pair, "ny": nm_y}
    for name in ORDER:
        stage, operands = (extra[name], ()) if name in extra else (stages[name[0]], (int(name[1]),))
        stage(*operands)
    arrive(held["nm_y"])
    arrive(shared)
    for copy in sent:
        copy.wait_send()


def write(nm, cc, new_p, new_m, out, buf_p, buf_m, sem):
    zh, x, c = (lax.axis_index(a) for a in SHARD)
    copies = [pltpu.make_async_copy(cc.at[h], out.at[h], sem.at[h]) for h in range(4)]
    for copy in copies:
        copy.start()
    buf_p[...] = cc[zh, x, c].astype(F32)
    copies.append(pltpu.make_async_copy(buf_p, new_p, sem.at[4]))
    copies[4].start()
    for t in range(4):
        for s in range(2):
            for q in range(NQ):
                cols = slice(q * COLS + s * 128, q * COLS + s * 128 + 128)
                value = nm[t, s, :, q * 128 : q * 128 + 128].astype(F32)
                buf_m[t * 16 : t * 16 + 16, cols] = value
    copies.append(pltpu.make_async_copy(buf_m, new_m, sem.at[5]))
    copies[5].start()
    for copy in copies:
        copy.wait()


def per_device(activations, cotangents, inner_params, inner_moment, outer_params, momentum):
    vmem = pl.BlockSpec(memory_space=pltpu.VMEM)
    hbm = pl.BlockSpec(memory_space=pltpu.HBM)
    whole = (4, 4, 2, 64, 1024)
    nm, cc = pl.pallas_call(
        kernel,
        out_shape=(pltpu.VMEM((4, 2, 16, NQ * 128), BF16), pltpu.VMEM(whole, BF16)),
        in_specs=[hbm] * 6,
        out_specs=(vmem, vmem),
        scratch_shapes=[
            pltpu.VMEM((4, 1024, 512), BF16),
            pltpu.VMEM((2, 1024, 512), BF16),
            pltpu.VMEM((4, 2, NQ, 4, 64, COLS), BF16),
            pltpu.VMEM((4, NQ, 4, 64, COLS), BF16),
            pltpu.VMEM((NQ, 2, 2, 64, COLS), BF16),
            pltpu.VMEM((NQ, 2, 2, 64, COLS), BF16),
            pltpu.VMEM((NQ, 2, 2, 64, COLS), BF16),
            pltpu.VMEM((NQ, 4, 64, COLS), BF16),
            pltpu.VMEM((NQ, 4, 4, 16, COLS), BF16),
            pltpu.VMEM((NQ, 3, 4, 16, COLS), BF16),
            pltpu.VMEM((NQ, 8, 16, 128), BF16),
            pltpu.VMEM((NQ, 7, 16, 128), BF16),
            pltpu.VMEM((1, 64, 1024), F32),
            pltpu.VMEM((1, 64, 1024), F32),
            pltpu.VMEM((64, 1024), F32),
            pltpu.VMEM((64, 1024), F32),
            pltpu.VMEM((4, 2, 16, NQ * 128), F32),
            pltpu.VMEM((3, 2, 16, NQ * 128), F32),
            pltpu.VMEM((2, 16, NQ * 128), F32),
            pltpu.VMEM((16, NQ * 128), F32),
            pltpu.VMEM((64, COLS), F32),
            pltpu.VMEM((2, 2, 64, COLS), BF16),
            pltpu.VMEM((2, 2, 64, COLS), BF16),
            pltpu.VMEM((2, 2, 64, COLS), BF16),
            pltpu.VMEM((4, 64, COLS), BF16),
            pltpu.VMEM((3, 64, COLS), BF16),
            pltpu.VMEM((4, 2, 16, 128), BF16),
            pltpu.SemaphoreType.DMA((32,)),
            pltpu.SemaphoreType.DMA((SEMS,)),
            pltpu.SemaphoreType.DMA((SEMS,)),
        ],
        compiler_params=pltpu.CompilerParams(
            collective_id=0, has_side_effects=True, vmem_limit_bytes=61100 * 1024
        ),
    )(activations, cotangents, inner_params, inner_moment, outer_params, momentum)
    new_p, new_m, out = pl.pallas_call(
        write,
        out_shape=(
            jax.ShapeDtypeStruct((64, 1024), F32),
            jax.ShapeDtypeStruct((64, 1024), F32),
            jax.ShapeDtypeStruct(whole, BF16),
        ),
        in_specs=[vmem, vmem],
        out_specs=(hbm, hbm, hbm),
        scratch_shapes=[
            pltpu.VMEM((64, 1024), F32),
            pltpu.VMEM((64, 1024), F32),
            pltpu.SemaphoreType.DMA((6,)),
        ],
        compiler_params=pltpu.CompilerParams(vmem_limit_bytes=8 * 2**20),
    )(nm, cc)
    return new_p, new_m, out.reshape(2048, 1024)


def solution(mesh):
    split = Mesh(mesh.devices.reshape(*(SIZE[a] for a in AXES)), AXES)
    return jax.shard_map(
        per_device,
        mesh=split,
        in_specs=(
            P(AXES, None),
            P(AXES, None),
            P(REP, SHARD, None),
            P(REP, SHARD, None),
            P(SHARD, None),
            P(SHARD, None),
        ),
        out_specs=(P(SHARD, None), P(SHARD, None), P()),
        check_vma=False,
    )
```
